256 devices in a mesh: groups: 2 (over y), pool: 64 (over z, x), heads: 2 (over core).
Axes of the slice: x: 4, y: 2, z: 16, core: 2. Of those that a mesh axis runs over, the one named last changes fastest.
The devices are a block of a 4x16x16 slice.
Arguments:
- hidden_in: bfloat16 [32, 8192], P('groups'), parts along dimension 0, may hold values from -50 to 50
- key_cache: bfloat16 [32, 8, 4096, 128], P('groups', 'heads', 'pool'), parts along dimension 0, may hold values from -200 to 200
- value_cache: bfloat16 [32, 8, 4096, 128], P('groups', 'heads', 'pool'), parts along dimension 0, may hold values from -6 to 6
- positions: int32 [3, 32, 4096], P(None, 'groups', 'pool'), parts along dimension 1, may hold values from 0 to 4095, as said below
- query_pos: int32 [3, 32], P(None, 'groups'), parts along dimension 1, may hold values from 4096 to 8207
- lengths: int32 [32], P('groups'), parts along dimension 0, may hold values from 1024 to 4096, as said below
- query_weight: bfloat16 [8192, 8192], P('pool', 'heads'), may hold values from -0.0625 to 0.0625
- key_weight: bfloat16 [8192, 1024], P('pool', 'heads'), may hold values from -0.16503906 to 0.16503906
- value_weight: bfloat16 [8192, 1024], P('pool', 'heads'), may hold values from -0.16503906 to 0.16503906
- out_weight: bfloat16 [8192, 8192], P('heads', 'pool'), may hold values from -0.5 to 0.5
- gate_weight: bfloat16 [8192, 14848], P(None, ('pool', 'heads')), may hold values from -0.0625 to 0.0625
- up_weight: bfloat16 [8192, 14848], P(None, ('pool', 'heads')), may hold values from -0.0625 to 0.0625
- down_weight: bfloat16 [14848, 8192], P(('pool', 'heads')), may hold values from -0.1875 to 0.1875
Outputs:
- output: bfloat16 [32, 8192], P('groups', 'pool'), parts along dimension 0
The draws below stay inside these ranges and needn't reach their ends.
There are 2 independent parts, one for each index of `groups`. The reference program is written for one: setup_inputs(seed, part) draws one part's arguments, and reference() takes and returns one part's arrays. A program takes and returns all parts, laid end to end along the dimension named above; an argument that names none is the same for every part. Nothing has to cross between parts.
Inputs may be any that keep to these rules, and one draw needn't show every extreme that they name: `positions`: text tokens carry three equal ids; one prompt is text only. `lengths`: some prompt fills all 4096 slots.
All inputs are finite; a program needn't handle non-finite values.
Results may differ from the reference program's by a relative error of at most 0.007.
The reference program's roundings to bfloat16 on the way count: a program that leaves them out, or rounds other values in their place, can miss the bound.
Values may be sent and summed in bfloat16 or wider, within the bound.
A program may use at most 64 MiB of HBM per device.

```python
import math
import jax
import jax.numpy as jnp
from jax import lax

D = 8192
HEADS = 64
KV_HEADS = 8
HD = 128
FF = 14848
PROMPTS = 16
SEQ = 4096


def draw_hidden_in(key, part):
    subkeys = jax.random.split(jax.random.fold_in(key, 11), 3)
    values_base = jax.random.truncated_normal(subkeys[0], -4.0, 4.0, (PROMPTS, D), jnp.float32)
    row_scale = jnp.exp(jax.random.uniform(subkeys[1], (PROMPTS, 1), jnp.float32, 0.0, math.log(4.0)))
    rise = math.log(10.0)
    column = jnp.arange(D).astype(jnp.float32) / D
    col_scale = jnp.exp(rise * (column - 0.5) + jax.random.uniform(subkeys[2], (D,), jnp.float32, -0.4, 0.4))
    return jnp.clip(values_base * row_scale * col_scale[None, :], -50.0, 50.0).astype(jnp.bfloat16)


def draw_key_cache(key, part):
    subkeys = jax.random.split(jax.random.fold_in(key, 53), 4)
    full_shape = (PROMPTS, KV_HEADS, SEQ, HD)
    base_values = 2.0 * jax.random.truncated_normal(subkeys[0], -6.0, 6.0, full_shape, jnp.float32)
    strength = jnp.exp(jax.random.uniform(subkeys[1], (PROMPTS, KV_HEADS, 1, 1), jnp.float32, math.log(30.0), math.log(200.0)))
    pattern = jax.random.rademacher(subkeys[2], (PROMPTS, KV_HEADS, 1, HD), jnp.float32)
    slot_choice = jax.random.randint(subkeys[3], (3, PROMPTS, KV_HEADS, 1, 1), 0, SEQ // 4)
    slot_index = jnp.arange(SEQ).reshape(1, 1, SEQ, 1)
    drawn = base_values
    for planted_index, factor in enumerate((1.0, 0.99, 0.98)):
        drawn = jnp.where(slot_index == slot_choice[planted_index], factor * strength * pattern, drawn)
    return jnp.clip(drawn, -200.0, 200.0).astype(jnp.bfloat16)


def draw_positions(key, part):
    subkeys = jax.random.split(jax.random.fold_in(key, 23), 3)
    text_len = jax.random.randint(subkeys[0], (PROMPTS,), 4, max(5, SEQ // 4))
    step_size = jax.random.randint(subkeys[1], (PROMPTS,), 1, 5)
    text_prompt = jax.random.randint(subkeys[2], (), 0, PROMPTS)
    token_index = jnp.arange(SEQ)[None, :]
    offset = token_index - text_len[:, None]
    in_video = (offset >= 0) & (jnp.arange(PROMPTS)[:, None] != text_prompt)
    clamped = jnp.maximum(offset, 0)
    frame = clamped // 64
    patch_row = clamped % 64 // 8
    patch_col = clamped % 8
    temporal = jnp.where(in_video, text_len[:, None] + frame * step_size[:, None], token_index)
    height = jnp.where(in_video, text_len[:, None] + patch_row, token_index)
    width = jnp.where(in_video, text_len[:, None] + patch_col, token_index)
    return jnp.clip(jnp.stack([temporal, height, width]), 0, SEQ - 1).astype(jnp.int32)


def draw_query_pos(key, part):
    subkeys = jax.random.split(jax.random.fold_in(key, 37), 2)
    anchor = jax.random.randint(subkeys[0], (1, PROMPTS), SEQ, 2 * SEQ)
    extra = jax.random.randint(subkeys[1], (3, PROMPTS), 0, 16)
    return (anchor + extra).astype(jnp.int32)


def draw_lengths(key, part):
    subkeys = jax.random.split(jax.random.fold_in(key, 41), 2)
    drawn = jax.random.randint(subkeys[0], (PROMPTS,), SEQ // 4, SEQ + 1)
    chosen = jax.random.randint(subkeys[1], (), 0, PROMPTS)
    return drawn.at[chosen].set(SEQ).astype(jnp.int32)


def spiked(values, rng, source, target, shards_of, factor):
    def block_of(axis_at):
        return (jnp.arange(values.shape[axis_at]) // (values.shape[axis_at] // shards_of)).reshape((-1,) + (1,) * (values.ndim - 1 - axis_at))

    one_side = jax.random.permutation(rng, shards_of)[block_of(target)]
    far = (block_of(target) + shards_of // 2) % shards_of
    return jnp.where((block_of(source) == one_side) | (block_of(source) == far), factor * values, values)


def block_levels(rng, shape, shards, low, high):
    gain, own = 1.0, jax.random.fold_in(rng, 6)
    for axis_at, shards_of in shards:
        draws = jnp.exp(jax.random.uniform(jax.random.fold_in(own, axis_at), (shards_of,), jnp.float32, low / len(shards), high / len(shards)))
        gain = gain * jnp.repeat(draws, shape[axis_at] // shards_of).reshape([-1 if axis == axis_at else 1 for axis in range(len(shape))])
    return gain


def centred(rng, dims, spread, most, shards=(), held_as=jnp.bfloat16):
    values = spread * jax.random.normal(rng, dims, jnp.float32)
    if shards:
        values = values * block_levels(rng, dims, shards, -0.22, 0.18)
    return jnp.clip(values, -most, most).astype(held_as)


def bell_draw_with(own_key, shape, spread, reach, shards, heavy, dtype=jnp.bfloat16):
    values = spread * jax.random.normal(own_key, shape, jnp.float32)
    if shards:
        values = values * block_levels(own_key, shape, shards, -0.22, 0.18)
    return jnp.clip(spiked(values, jax.random.fold_in(own_key, 3), *heavy), -reach, reach).astype(dtype)


def setup_inputs(seed: int = 0, part: int = 0) -> dict:
    arg_keys = jax.random.split(jax.random.key(seed), 14)
    part_keys = jax.random.split(jax.random.fold_in(arg_keys[13], part), 14)
    return {
        "hidden_in": draw_hidden_in(jax.random.fold_in(jax.random.fold_in(arg_keys[13], part), 71), part),
        "key_cache": draw_key_cache(jax.random.fold_in(jax.random.fold_in(arg_keys[13], part), 71), part),
        "value_cache": centred(part_keys[2], (PROMPTS, KV_HEADS, SEQ, HD), 1.0, 6.0, ((1, 2), (2, 64))),
        "positions": draw_positions(jax.random.fold_in(jax.random.fold_in(arg_keys[13], part), 71), part),
        "query_pos": draw_query_pos(jax.random.fold_in(jax.random.fold_in(arg_keys[13], part), 71), part),
        "lengths": draw_lengths(jax.random.fold_in(jax.random.fold_in(arg_keys[13], part), 71), part),
        "query_weight": centred(arg_keys[6], (D, HEADS * HD), D ** -0.5, 0.0625, ((0, 64), (1, 2))),
        "key_weight": centred(arg_keys[7], (D, KV_HEADS * HD), (2.5 / D ** 0.5), 0.16503906, ((0, 64), (1, 2))),
        "value_weight": centred(arg_keys[8], (D, KV_HEADS * HD), (2.5 / D ** 0.5), 0.16503906, ((0, 64), (1, 2))),
        "out_weight": centred(arg_keys[9], (HEADS * HD, D), HD ** -0.5, 0.5, ((0, 2), (1, 64))),
        "gate_weight": centred(arg_keys[10], (D, FF), D ** -0.5, 0.0625, ((1, 128),)),
        "up_weight": centred(arg_keys[11], (D, FF), D ** -0.5, 0.0625, ((1, 128),)),
        "down_weight": bell_draw_with(arg_keys[12], (FF, D), FF ** -0.5, 0.1875, ((0, 128),), (0, 1, 128, 5.5)),
    }


EPS = 1e-06
THETA = 1000000.0

def angle_tables(triple):
    half_dim = HD // 2
    column = jnp.arange(half_dim)
    first_end = HD // 8
    second_end = first_end + 3 * HD // 16
    chosen = jnp.where(column < first_end, triple[0][..., None], jnp.where(column < second_end, triple[1][..., None], triple[2][..., None]))
    inverse = jnp.exp(column.astype(jnp.float32) * (-2.0 * math.log(THETA) / HD))
    angles = chosen.astype(jnp.float32) * inverse
    return (jnp.cos(angles), jnp.sin(angles))

def rotate(values, cos_table, sin_table):
    half_dim = values.shape[-1] // 2
    lower_half = values[..., :half_dim]
    upper_half = values[..., half_dim:]
    return jnp.concatenate([lower_half * cos_table - upper_half * sin_table, upper_half * cos_table + lower_half * sin_table], -1)

def normalize(values):
    return values * lax.rsqrt(lax.optimization_barrier(jnp.mean(values * values, -1, keepdims=True)) + EPS)

def reference(hidden_in, key_cache, value_cache, positions, query_pos, lengths, query_weight, key_weight, value_weight, out_weight, gate_weight, up_weight, down_weight):
    group_size = HEADS // KV_HEADS
    score_scale = HD ** (-0.5)
    normed = normalize(hidden_in.astype(jnp.float32)).astype(jnp.bfloat16)
    raw_queries = jnp.dot(normed, query_weight, preferred_element_type=jnp.float32).reshape(PROMPTS, HEADS, HD)
    raw_keys = jnp.dot(normed, key_weight, preferred_element_type=jnp.float32).reshape(PROMPTS, KV_HEADS, HD)
    new_values = jnp.dot(normed, value_weight, preferred_element_type=jnp.float32).reshape(PROMPTS, KV_HEADS, HD).astype(jnp.bfloat16)
    query_cos, query_sin = angle_tables(query_pos)
    queries = rotate(raw_queries, query_cos[:, None], query_sin[:, None]).astype(jnp.bfloat16)
    own_keys = rotate(raw_keys, query_cos[:, None], query_sin[:, None]).astype(jnp.bfloat16)

    def attend_prompt(inputs):
        query_rows, key_new, value_new, cached_keys, cached_values, triple, length = inputs
        cos_table, sin_table = angle_tables(triple)
        rotated = rotate(cached_keys.astype(jnp.float32), cos_table[None], sin_table[None]).astype(jnp.bfloat16)
        grouped = query_rows.reshape(KV_HEADS, group_size, HD).astype(jnp.float32)
        scores = jnp.einsum('kgd,ksd->kgs', grouped, rotated.astype(jnp.float32)) * score_scale
        valid_mask = jnp.arange(SEQ) < length
        scores = jnp.where(valid_mask, scores, -1e+30)
        own_score = jnp.einsum('kgd,kd->kg', grouped, key_new.astype(jnp.float32)) * score_scale
        peak_score = jnp.maximum(lax.optimization_barrier(jnp.max(scores, -1)), own_score)
        weights = jnp.where(valid_mask, jnp.exp(scores - peak_score[..., None]), 0.0)
        own_weight = jnp.exp(own_score - peak_score)
        denominator = lax.optimization_barrier(jnp.sum(weights, -1)) + own_weight
        blended = jnp.einsum('kgs,ksd->kgd', weights, cached_values.astype(jnp.float32))
        blended = blended + own_weight[..., None] * value_new.astype(jnp.float32)[:, None, :]
        return (blended / denominator[..., None]).reshape(HEADS * HD).astype(jnp.bfloat16)
    triples = jnp.transpose(positions, (1, 0, 2))
    attended = lax.map(attend_prompt, (queries, own_keys, new_values, key_cache, value_cache, triples, lengths))
    attn_out = jnp.dot(attended, out_weight, preferred_element_type=jnp.float32)
    mid_state = (hidden_in.astype(jnp.float32) + attn_out).astype(jnp.bfloat16)
    normed_state = normalize(mid_state.astype(jnp.float32)).astype(jnp.bfloat16)
    gate_values = jnp.dot(normed_state, gate_weight, preferred_element_type=jnp.float32)
    up_values = jnp.dot(normed_state, up_weight, preferred_element_type=jnp.float32)
    active = (jax.nn.silu(gate_values) * up_values).astype(jnp.bfloat16)
    down_values = jnp.dot(active, down_weight, preferred_element_type=jnp.float32)
    return (mid_state.astype(jnp.float32) + down_values).astype(jnp.bfloat16)
```

```python
import functools
import math

import jax
import jax.numpy as jnp
from jax import lax
from jax.experimental import pallas as pl
from jax.experimental.pallas import tpu as pltpu
from jax.sharding import PartitionSpec as P

HD = 128
EPS = 1e-06
THETA = 1000000.0
NX = 4
MESH = pl.DeviceIdType.MESH
F32 = jnp.float32
BF16 = jnp.bfloat16


def far_first(pool):
    nz = pool // NX
    steps = [(a, b) for a in range(nz) for b in range(NX) if (a, b) != (0, 0)]
    return sorted(steps, key=lambda s: -(min(s[0], nz - s[0]) + min(s[1], NX - s[1])))


def rotate(values, cos_table, sin_table):
    return values * cos_table + pltpu.roll(values, HD // 2, values.ndim - 1) * sin_table


def choose_ids(lane, t, h, w):
    column = lane % (HD // 2)
    first_end = HD // 8
    second_end = first_end + 3 * HD // 16
    return jnp.where(column < first_end, t, jnp.where(column < second_end, h, w))


def inverse_row(lane):
    column = (lane % (HD // 2)).astype(F32)
    return jnp.exp(column * (-2.0 * math.log(THETA) / HD))


def body(
    cfg,
    query_pos,
    lengths,
    hidden_hbm,
    key_hbm,
    value_hbm,
    positions,
    qw_hbm,
    kw_hbm,
    vw_hbm,
    ow_hbm,
    gw_hbm,
    uw_hbm,
    dw_hbm,
    out_ref,
    hidden,
    keys,
    values,
    qw,
    kw,
    vw,
    ow,
    gw,
    uw,
    dw,
    term,
    term_in,
    item,
    item_in,
    q_send,
    q_all,
    pos_t,
    o_send,
    o_in,
    lse_send,
    lse_in,
    lse_t,
    att_send,
    att_all,
    att_rows,
    att_lhs,
    hid_cols,
    proj,
    proj_in,
    mid_send,
    mid_all,
    normed_lhs,
    down,
    down_in,
    down_send,
    part_in,
    fin,
    load_sem,
    send_sem,
    recv_sem,
):
    prompts, pool, kv, group, slots = cfg
    nz = pool // NX
    group_i = lax.axis_index("groups")
    me = lax.axis_index("pool")
    core = lax.axis_index("heads")
    z = me // NX
    x = me % NX
    half = prompts // 2
    steps = far_first(pool)

    def at(dz, dx):
        return lax.rem(z + dz, nz) * NX + lax.rem(x + dx, NX)

    def dev(p):
        return (group_i, p, core)

    other = (group_i, me, 1 - core)

    loads = []
    for n, (src, dst) in enumerate(
        [
            (hidden_hbm, hidden),
            (qw_hbm, qw),
            (kw_hbm, kw),
            (vw_hbm, vw),
            (key_hbm, keys),
            (value_hbm, values),
            (ow_hbm, ow),
            (gw_hbm, gw),
            (uw_hbm, uw),
            (dw_hbm, dw),
        ]
    ):
        copy = pltpu.make_async_copy(src, dst, load_sem.at[n])
        copy.start()
        loads.append(copy)

    barrier = pltpu.get_barrier_semaphore()
    for dz, dx in steps:
        pl.semaphore_signal(barrier, inc=1, device_id=dev(at(dz, dx)), device_id_type=MESH)
    pl.semaphore_signal(barrier, inc=1, device_id=other, device_id_type=MESH)

    def send(src, dst, n, device):
        pltpu.make_async_remote_copy(
            src_ref=src,
            dst_ref=dst,
            send_sem=send_sem.at[n],
            recv_sem=recv_sem.at[n],
            device_id=device,
            device_id_type=MESH,
        ).start()

    def arrived(view, n):
        pltpu.make_async_copy(view, view, recv_sem.at[n]).wait()

    def sent(view, n):
        pltpu.make_async_copy(view, view, send_sem.at[n]).wait()

    loads[0].wait()
    wide = hidden[...].astype(F32)
    scale = lax.rsqrt(jnp.mean(wide * wide, -1, keepdims=True) + EPS)
    mine = hidden[:, pl.ds(pl.multiple_of(me * HD, HD), HD)].astype(F32)
    hid_cols[...] = mine
    normed_cols = (mine * scale).astype(BF16)
    for n in (1, 2, 3):
        loads[n].wait()
    width = group * HD
    for dx in (2, 1, 3, 0):
        g = lax.rem(x + dx, NX)
        part = jnp.dot(
            normed_cols,
            qw[:, pl.ds(pl.multiple_of(g * width, width), width)],
            preferred_element_type=F32,
        )
        for j in range(group):
            term[g, j] = part[:, j * HD : (j + 1) * HD]
        columns = pl.ds(pl.multiple_of(g * HD, HD), HD)
        term[g, group] = jnp.dot(normed_cols, kw[:, columns], preferred_element_type=F32)
        term[g, group + 1] = jnp.dot(normed_cols, vw[:, columns], preferred_element_type=F32)

    pl.semaphore_wait(barrier, pool)

    for dx in (2, 1, 3):
        g = lax.rem(x + dx, NX)
        send(term.at[g], term_in.at[dx - 1], 0, dev(at(0, dx)))

    wide_pos = jnp.concatenate(
        [positions[k].astype(F32) for k in range(3)]
        + [jnp.zeros((HD - 3 * prompts, slots), F32)],
        0,
    )
    wide_pos = jnp.concatenate([wide_pos, jnp.zeros((HD, HD - slots), F32)], 1)
    pos_t[...] = wide_pos.T

    arrived(term_in, 0)
    for j in range(group + 2):
        item[:, j, :] = term[x, j] + term_in[0, j] + term_in[1, j] + term_in[2, j]

    for dz in sorted(range(1, nz), key=lambda d: -min(d, nz - d)):
        p = lax.rem(z + dz, nz)
        send(item.at[p], item_in.at[dz - 1], 1, dev(at(dz, 0)))

    loads[4].wait()
    lane = lax.broadcasted_iota(jnp.int32, (slots, HD), 1)
    inv = inverse_row(lane)
    sign = jnp.where(lane < HD // 2, -1.0, 1.0)

    for p in range(prompts):
        ids = choose_ids(
            lane,
            pos_t[0:slots, p : p + 1],
            pos_t[0:slots, prompts + p : prompts + p + 1],
            pos_t[0:slots, 2 * prompts + p : 2 * prompts + p + 1],
        )
        angles = ids * inv
        cos_table = jnp.cos(angles)
        sin_table = jnp.sin(angles) * sign
        for g in range(kv):
            keys[p, g] = rotate(keys[p, g].astype(F32), cos_table, sin_table).astype(BF16)

    arrived(item_in, 1)
    total = item[z]
    for d in range(nz - 1):
        total = total + item_in[d]

    row = lax.broadcasted_iota(jnp.int32, (1, HD), 1)
    ids = choose_ids(
        row,
        query_pos[0, z].astype(F32),
        query_pos[1, z].astype(F32),
        query_pos[2, z].astype(F32),
    )
    angles = ids * inverse_row(row)
    cos_row = jnp.cos(angles)
    sin_row = jnp.sin(angles) * jnp.where(row < HD // 2, -1.0, 1.0)
    my_queries = rotate(total[0:group], cos_row, sin_row).astype(BF16)
    my_key = rotate(total[group : group + 1], cos_row, sin_row).astype(BF16).astype(F32)
    my_value = total[group + 1 : group + 2].astype(BF16).astype(F32)

    q_send[...] = my_queries
    for dz, dx in steps:
        send(q_send, q_all.at[me], 2, dev(at(dz, dx)))
    q_all[me] = my_queries
    loads[5].wait()
    arrived(q_all.at[pl.ds(0, pool - 1)], 2)

    rows = kv * group
    r_i = lax.broadcasted_iota(jnp.int32, (rows, kv * slots), 0)
    c_i = lax.broadcasted_iota(jnp.int32, (rows, kv * slots), 1)
    diagonal = r_i // group == c_i // slots
    slot = c_i % slots + me * slots
    eye = lax.broadcasted_iota(jnp.int32, (rows, HD), 0) == lax.broadcasted_iota(
        jnp.int32, (rows, HD), 1
    )
    for dz in sorted(range(nz), key=lambda d: -min(d, nz - d)):
        p = lax.rem(z + dz, nz)
        first = p * kv
        q4 = q_all[pl.ds(first, kv)].astype(F32).reshape(rows, HD).astype(BF16)
        k4 = keys[p].reshape(kv * slots, HD)
        v4 = values[p].reshape(kv * slots, HD)
        scores = lax.dot_general(
            q4, k4, (((1,), (1,)), ((), ())), preferred_element_type=F32
        ) * HD ** (-0.5)
        valid = diagonal & (slot < lengths[p])
        scores = jnp.where(valid, scores, -1e30)
        peak = jnp.max(scores, -1, keepdims=True)
        weights = jnp.where(valid, jnp.exp(scores - peak), 0.0).astype(BF16)
        norm = jnp.sum(weights.astype(F32), -1, keepdims=True)
        some = norm > 0.0
        lse = jnp.where(some, peak + jnp.log(jnp.where(some, norm, 1.0)), -1e30)
        blended = jnp.dot(weights, v4, preferred_element_type=F32)
        blended = blended / jnp.where(some, norm, 1.0)
        o_send[pl.ds(first, kv)] = blended.reshape(kv, group, HD).astype(BF16)
        lse_send[p] = jnp.sum(jnp.where(eye, lse, 0.0), 0, keepdims=True)
        for dx in (2, 1, 3, 0):
            if dz == 0 and dx == 0:
                continue
            to = at(dz, dx)
            slot_there = dz * NX + dx - 1
            send(lse_send.at[p], lse_in.at[slot_there], 3, dev(to))
            send(o_send.at[to], o_in.at[slot_there], 4, dev(to))

    own_score = jnp.sum(my_queries.astype(F32) * my_key, -1, keepdims=True) * HD ** (-0.5)

    o_in[pool - 1] = o_send[me]
    lse_in[pool - 1] = lse_send[z]
    arrived(lse_in.at[pl.ds(0, pool - 1)], 3)
    lse_rows = lse_in[...].reshape(pool, HD)
    lse_t[...] = jnp.concatenate([lse_rows, jnp.full((HD - pool, HD), -1e30, F32)], 0).T
    lse = lse_t[pl.ds(pl.multiple_of(x * group, group), group), :]
    top = jnp.maximum(jnp.max(lse, -1, keepdims=True), own_score)
    factor = jnp.exp(lse - top)
    own_weight = jnp.exp(own_score - top)
    denominator = jnp.sum(factor, -1, keepdims=True) + own_weight
    factor = factor / denominator
    own_weight = own_weight / denominator
    arrived(o_in.at[pl.ds(0, pool - 1)], 4)
    mixed = [own_weight * my_value, None, None, None]
    for s in range(pool):
        piece = factor[:, s : s + 1] * o_in[s].astype(F32)
        k = s % 4
        mixed[k] = piece if mixed[k] is None else mixed[k] + piece
    attended = ((mixed[0] + mixed[1]) + (mixed[2] + mixed[3])).astype(BF16)

    att_send[...] = attended
    for dz, dx in steps:
        send(att_send, att_all.at[me], 5, dev(at(dz, dx)))
    att_all[me] = attended
    loads[6].wait()
    arrived(att_all.at[pl.ds(0, pool - 1)], 5)
    att_rows[...] = att_all[...].astype(F32).reshape(pool * group, HD)
    for j in range(rows):
        att_lhs[:, j * HD : (j + 1) * HD] = att_rows[
            pl.ds(j, prompts, stride=rows), :
        ].astype(BF16)
    projected = jnp.dot(att_lhs[...], ow[...], preferred_element_type=F32)

    proj[0] = projected[0:half]
    proj[1] = projected[half:prompts]
    send(proj.at[1 - core], proj_in, 6, other)
    arrived(proj_in, 6)
    mid = (
        hid_cols[pl.ds(pl.multiple_of(core * half, half), half), :] + proj[core] + proj_in[...]
    ).astype(BF16)

    mid_send[...] = mid
    for dz, dx in steps:
        send(mid_send, mid_all.at[core, me], 7, dev(at(dz, dx)))
    mid_all[core, me] = mid
    arrived(mid_all.at[0, pl.ds(0, pool - 1)], 7)
    send(mid_all.at[core], mid_all.at[core], 8, other)
    arrived(mid_all.at[0], 8)

    inverse = []
    for c in range(2):
        state = mid_all[c].astype(F32)
        squares = jnp.sum(jnp.sum(state * state, 0), -1, keepdims=True)
        inverse.append(lax.rsqrt(squares * (1.0 / (pool * HD)) + EPS))
    for k in range(pool):
        chunk = jnp.concatenate([mid_all[c, k].astype(F32) * inverse[c] for c in range(2)], 0)
        normed_lhs[:, k * HD : (k + 1) * HD] = chunk.astype(BF16)
    loads[7].wait()
    loads[8].wait()
    gate = jnp.dot(normed_lhs[...], gw[...], preferred_element_type=F32)
    up = jnp.dot(normed_lhs[...], uw[...], preferred_element_type=F32)
    active = (gate / (1.0 + jnp.exp(-gate)) * up).astype(BF16)

    loads[9].wait()
    wide_cols = 8 * HD
    for c in range(pool // 8):
        part = jnp.dot(
            active, dw[:, c * wide_cols : (c + 1) * wide_cols], preferred_element_type=F32
        )
        for k in range(8):
            down[0, c * 8 + k] = part[0:half, k * HD : (k + 1) * HD]
            down[1, c * 8 + k] = part[half:prompts, k * HD : (k + 1) * HD]
    send(down.at[1 - core], down_in, 9, other)
    arrived(down_in, 9)
    down_send[...] = (down[core] + down_in[...]).astype(BF16)
    for dz, dx in steps:
        to = at(dz, dx)
        send(down_send.at[to], part_in.at[dz * NX + dx - 1], 10, dev(to))
    part_in[pool - 1] = down_send[me]
    arrived(part_in.at[pl.ds(0, pool - 1)], 10)
    done = mid.astype(F32) + jnp.sum(part_in[...].astype(F32), 0)
    fin[core] = done.astype(BF16)
    send(fin.at[core], fin.at[core], 11, other)
    arrived(fin.at[0], 11)
    out_ref[...] = jnp.concatenate([fin[0].astype(F32), fin[1].astype(F32)], 0).astype(BF16)

    sent(term_in, 0)
    sent(item_in, 1)
    sent(q_all.at[pl.ds(0, pool - 1)], 2)
    sent(lse_in.at[pl.ds(0, pool - 1)], 3)
    sent(o_in.at[pl.ds(0, pool - 1)], 4)
    sent(att_all.at[pl.ds(0, pool - 1)], 5)
    sent(proj_in, 6)
    sent(mid_all.at[0, pl.ds(0, pool - 1)], 7)
    sent(mid_all.at[0], 8)
    sent(down_in, 9)
    sent(part_in.at[pl.ds(0, pool - 1)], 10)
    sent(fin.at[0], 11)


def solution(mesh):
    pool = mesh.shape["pool"]

    def per_device(
        hidden_in,
        key_cache,
        value_cache,
        positions,
        query_pos,
        lengths,
        query_weight,
        key_weight,
        value_weight,
        out_weight,
        gate_weight,
        up_weight,
        down_weight,
    ):
        prompts, kv, slots, _ = key_cache.shape
        group = query_weight.shape[1] // (kv * HD)
        nz = pool // NX
        parts = group + 2
        half = prompts // 2
        hbm = pl.BlockSpec(memory_space=pltpu.HBM)
        vmem = pl.BlockSpec(memory_space=pltpu.VMEM)
        smem = pl.BlockSpec(memory_space=pltpu.SMEM)

        def like(a):
            return pltpu.VMEM(a.shape, a.dtype)

        scratch = [
            like(hidden_in),
            like(key_cache),
            like(value_cache),
            like(query_weight),
            like(key_weight),
            like(value_weight),
            like(out_weight),
            like(gate_weight),
            like(up_weight),
            like(down_weight),
            pltpu.VMEM((kv, parts, prompts, HD), F32),
            pltpu.VMEM((NX - 1, parts, prompts, HD), F32),
            pltpu.VMEM((prompts, parts, HD), F32),
            pltpu.VMEM((nz - 1, parts, HD), F32),
            pltpu.VMEM((group, HD), BF16),
            pltpu.VMEM((pool, group, HD), BF16),
            pltpu.VMEM((HD, HD), F32),
            pltpu.VMEM((pool, group, HD), BF16),
            pltpu.VMEM((pool, group, HD), BF16),
            pltpu.VMEM((prompts, 1, HD), F32),
            pltpu.VMEM((pool, 1, HD), F32),
            pltpu.VMEM((HD, HD), F32),
            pltpu.VMEM((group, HD), BF16),
            pltpu.VMEM((pool, group, HD), BF16),
            pltpu.VMEM((pool * group, HD), F32),
            pltpu.VMEM((prompts, kv * group * HD), BF16),
            pltpu.VMEM((prompts, HD), F32),
            pltpu.VMEM((2, half, HD), F32),
            pltpu.VMEM((half, HD), F32),
            pltpu.VMEM((half, HD), BF16),
            pltpu.VMEM((2, pool, half, HD), BF16),
            pltpu.VMEM((prompts, pool * HD), BF16),
            pltpu.VMEM((2, pool, half, HD), F32),
            pltpu.VMEM((pool, half, HD), F32),
            pltpu.VMEM((pool, half, HD), BF16),
            pltpu.VMEM((pool, half, HD), BF16),
            pltpu.VMEM((2, half, HD), BF16),
            pltpu.SemaphoreType.DMA((10,)),
            pltpu.SemaphoreType.DMA((12,)),
            pltpu.SemaphoreType.DMA((12,)),
        ]
        return pl.pallas_call(
            functools.partial(body, (prompts, pool, kv, group, slots)),
            out_shape=jax.ShapeDtypeStruct((prompts, HD), BF16),
            in_specs=[smem, smem, hbm, hbm, hbm, vmem] + [hbm] * 7,
            out_specs=vmem,
            scratch_shapes=scratch,
            compiler_params=pltpu.CompilerParams(
                collective_id=0, has_side_effects=True, vmem_limit_bytes=60 * 1024 * 1024
            ),
        )(
            query_pos,
            lengths,
            hidden_in,
            key_cache,
            value_cache,
            positions,
            query_weight,
            key_weight,
            value_weight,
            out_weight,
            gate_weight,
            up_weight,
            down_weight,
        )

    in_specs = (
        P("groups", None),
        P("groups", "heads", "pool", None),
        P("groups", "heads", "pool", None),
        P(None, "groups", "pool"),
        P(None, "groups"),
        P("groups"),
        P("pool", "heads"),
        P("pool", "heads"),
        P("pool", "heads"),
        P("heads", "pool"),
        P(None, ("pool", "heads")),
        P(None, ("pool", "heads")),
        P(("pool", "heads"), None),
    )
    return jax.shard_map(
        per_device, mesh=mesh, in_specs=in_specs, out_specs=P("groups", "pool"), check_vma=False
    )
```

```python
import functools
import math

import jax
import jax.numpy as jnp
from jax import lax
from jax.experimental import pallas as pl
from jax.experimental.pallas import tpu as pltpu
from jax.sharding import PartitionSpec as P

HD = 128
EPS = 1e-06
THETA = 1000000.0
NX = 4
MESH = pl.DeviceIdType.MESH
F32 = jnp.float32
BF16 = jnp.bfloat16


def far_first(pool):
    nz = pool // NX
    steps = [(a, b) for a in range(nz) for b in range(NX) if (a, b) != (0, 0)]
    return sorted(steps, key=lambda s: -(min(s[0], nz - s[0]) + min(s[1], NX - s[1])))


def rotate(values, cos_table, sin_table):
    return values * cos_table + pltpu.roll(values, HD // 2, values.ndim - 1) * sin_table


def choose_ids(lane, t, h, w):
    column = lane % (HD // 2)
    first_end = HD // 8
    second_end = first_end + 3 * HD // 16
    return jnp.where(column < first_end, t, jnp.where(column < second_end, h, w))


def inverse_row(lane):
    column = (lane % (HD // 2)).astype(F32)
    return jnp.exp(column * (-2.0 * math.log(THETA) / HD))


def body(
    cfg,
    query_pos,
    lengths,
    hidden_hbm,
    key_hbm,
    value_hbm,
    positions,
    qw_hbm,
    kw_hbm,
    vw_hbm,
    ow_hbm,
    gw_hbm,
    uw_hbm,
    dw_hbm,
    out_ref,
    hidden,
    keys,
    values,
    qw,
    kw,
    vw,
    ow,
    gw,
    uw,
    dw,
    term,
    term_in,
    item,
    item_in,
    q_send,
    q_all,
    pos_t,
    o_send,
    o_in,
    lse_send,
    lse_in,
    lse_t,
    att_send,
    att_all,
    att_rows,
    att_lhs,
    hid_cols,
    proj,
    proj_in,
    mid_send,
    mid_all,
    normed_lhs,
    down,
    down_in,
    down_send,
    part_in,
    fin,
    load_sem,
    send_sem,
    recv_sem,
    here_sem,
):
    prompts, pool, kv, group, slots = cfg
    nz = pool // NX
    group_i = lax.axis_index("groups")
    me = lax.axis_index("pool")
    core = lax.axis_index("heads")
    z = me // NX
    x = me % NX
    half = prompts // 2
    steps = far_first(pool)

    def at(dz, dx):
        return lax.rem(z + dz, nz) * NX + lax.rem(x + dx, NX)

    def dev(p):
        return (group_i, p, core)

    other = (group_i, me, 1 - core)

    barrier = pltpu.get_barrier_semaphore()
    near = [dev(at(0, dx)) for dx in (2, 1, 3)] + [dev(at(1, 0)), dev(at(nz - 1, 0)), other]
    for device in near:
        pl.semaphore_signal(barrier, inc=1, device_id=device, device_id_type=MESH)

    def tell(distance, n):
        for dz in (distance, nz - distance):
            pl.semaphore_signal(here_sem.at[n], inc=1, device_id=dev(at(dz, 0)), device_id_type=MESH)

    loads = []
    for n, (src, dst) in enumerate(
        [
            (hidden_hbm, hidden),
            (qw_hbm, qw),
            (kw_hbm, kw),
            (vw_hbm, vw),
            (key_hbm, keys),
            (value_hbm, values),
            (ow_hbm, ow),
            (gw_hbm, gw),
            (uw_hbm, uw),
            (dw_hbm, dw),
        ]
    ):
        copy = pltpu.make_async_copy(src, dst, load_sem.at[n])
        copy.start()
        loads.append(copy)


    def send(src, dst, n, device):
        pltpu.make_async_remote_copy(
            src_ref=src,
            dst_ref=dst,
            send_sem=send_sem.at[n],
            recv_sem=recv_sem.at[n],
            device_id=device,
            device_id_type=MESH,
        ).start()

    def arrived(view, n):
        pltpu.make_async_copy(view, view, recv_sem.at[n]).wait()

    def sent(view, n):
        pltpu.make_async_copy(view, view, send_sem.at[n]).wait()

    loads[0].wait()
    pl.semaphore_wait(barrier, len(near))
    tell(1, 0)
    wide = hidden[...].astype(F32)
    scale = lax.rsqrt(jnp.mean(wide * wide, -1, keepdims=True) + EPS)
    mine = hidden[:, pl.ds(pl.multiple_of(me * HD, HD), HD)].astype(F32)
    hid_cols[...] = mine
    normed_cols = (mine * scale).astype(BF16)
    for n in (1, 2, 3):
        loads[n].wait()
    width = group * HD
    for dx in (2, 1, 3, 0):
        g = lax.rem(x + dx, NX)
        part = jnp.dot(
            normed_cols,
            qw[:, pl.ds(pl.multiple_of(g * width, width), width)],
            preferred_element_type=F32,
        )
        for j in range(group):
            term[g, j] = part[:, j * HD : (j + 1) * HD]
        columns = pl.ds(pl.multiple_of(g * HD, HD), HD)
        term[g, group] = jnp.dot(normed_cols, kw[:, columns], preferred_element_type=F32)
        term[g, group + 1] = jnp.dot(normed_cols, vw[:, columns], preferred_element_type=F32)
        if dx:
            send(term.at[g], term_in.at[dx - 1], 0, dev(at(0, dx)))

    pl.semaphore_wait(here_sem.at[0], 2)
    tell(2, 1)
    pl.semaphore_wait(here_sem.at[1], 2)
    tell(4, 2)

    wide_pos = jnp.concatenate(
        [positions[k].astype(F32) for k in range(3)]
        + [jnp.zeros((HD - 3 * prompts, slots), F32)],
        0,
    )
    wide_pos = jnp.concatenate([wide_pos, jnp.zeros((HD, HD - slots), F32)], 1)
    pos_t[...] = wide_pos.T

    arrived(term_in, 0)
    for j in range(group + 2):
        item[:, j, :] = term[x, j] + term_in[0, j] + term_in[1, j] + term_in[2, j]

    pl.semaphore_wait(here_sem.at[2], 2)
    for dz in sorted(range(1, nz), key=lambda d: -min(d, nz - d)):
        p = lax.rem(z + dz, nz)
        send(item.at[p], item_in.at[dz - 1], 1, dev(at(dz, 0)))

    loads[4].wait()
    lane = lax.broadcasted_iota(jnp.int32, (slots, HD), 1)
    inv = inverse_row(lane)
    sign = jnp.where(lane < HD // 2, -1.0, 1.0)

    for p in range(prompts):
        ids = choose_ids(
            lane,
            pos_t[0:slots, p : p + 1],
            pos_t[0:slots, prompts + p : prompts + p + 1],
            pos_t[0:slots, 2 * prompts + p : 2 * prompts + p + 1],
        )
        angles = ids * inv
        cos_table = jnp.cos(angles)
        sin_table = jnp.sin(angles) * sign
        for g in range(kv):
            keys[p, g] = rotate(keys[p, g].astype(F32), cos_table, sin_table).astype(BF16)

    arrived(item_in, 1)
    total = item[z]
    for d in range(nz - 1):
        total = total + item_in[d]

    row = lax.broadcasted_iota(jnp.int32, (1, HD), 1)
    ids = choose_ids(
        row,
        query_pos[0, z].astype(F32),
        query_pos[1, z].astype(F32),
        query_pos[2, z].astype(F32),
    )
    angles = ids * inverse_row(row)
    cos_row = jnp.cos(angles)
    sin_row = jnp.sin(angles) * jnp.where(row < HD // 2, -1.0, 1.0)
    my_queries = rotate(total[0:group], cos_row, sin_row).astype(BF16)
    my_key = rotate(total[group : group + 1], cos_row, sin_row).astype(BF16).astype(F32)
    my_value = total[group + 1 : group + 2].astype(BF16).astype(F32)

    q_send[...] = my_queries
    for dz, dx in steps:
        send(q_send, q_all.at[me], 2, dev(at(dz, dx)))
    q_all[me] = my_queries
    loads[5].wait()
    arrived(q_all.at[pl.ds(0, pool - 1)], 2)

    rows = kv * group
    r_i = lax.broadcasted_iota(jnp.int32, (rows, kv * slots), 0)
    c_i = lax.broadcasted_iota(jnp.int32, (rows, kv * slots), 1)
    diagonal = r_i // group == c_i // slots
    slot = c_i % slots + me * slots
    eye = lax.broadcasted_iota(jnp.int32, (rows, HD), 0) == lax.broadcasted_iota(
        jnp.int32, (rows, HD), 1
    )
    for dz in sorted(range(nz), key=lambda d: -min(d, nz - d)):
        p = lax.rem(z + dz, nz)
        first = p * kv
        q4 = q_all[pl.ds(first, kv)].astype(F32).reshape(rows, HD).astype(BF16)
        k4 = keys[p].reshape(kv * slots, HD)
        v4 = values[p].reshape(kv * slots, HD)
        scores = lax.dot_general(
            q4, k4, (((1,), (1,)), ((), ())), preferred_element_type=F32
        ) * HD ** (-0.5)
        valid = diagonal & (slot < lengths[p])
        scores = jnp.where(valid, scores, -1e30)
        peak = jnp.max(scores, -1, keepdims=True)
        weights = jnp.where(valid, jnp.exp(scores - peak), 0.0).astype(BF16)
        norm = jnp.sum(weights.astype(F32), -1, keepdims=True)
        some = norm > 0.0
        lse = jnp.where(some, peak + jnp.log(jnp.where(some, norm, 1.0)), -1e30)
        blended = jnp.dot(weights, v4, preferred_element_type=F32)
        blended = blended / jnp.where(some, norm, 1.0)
        o_send[pl.ds(first, kv)] = blended.reshape(kv, group, HD).astype(BF16)
        lse_send[p] = jnp.sum(jnp.where(eye, lse, 0.0), 0, keepdims=True)
        for dx in (2, 1, 3, 0):
            if dz == 0 and dx == 0:
                continue
            to = at(dz, dx)
            slot_there = dz * NX + dx - 1
            send(lse_send.at[p], lse_in.at[slot_there], 3, dev(to))
            send(o_send.at[to], o_in.at[slot_there], 4, dev(to))

    own_score = jnp.sum(my_queries.astype(F32) * my_key, -1, keepdims=True) * HD ** (-0.5)

    o_in[pool - 1] = o_send[me]
    lse_in[pool - 1] = lse_send[z]
    arrived(lse_in.at[pl.ds(0, pool - 1)], 3)
    lse_rows = lse_in[...].reshape(pool, HD)
    lse_t[...] = jnp.concatenate([lse_rows, jnp.full((HD - pool, HD), -1e30, F32)], 0).T
    lse = lse_t[pl.ds(pl.multiple_of(x * group, group), group), :]
    top = jnp.maximum(jnp.max(lse, -1, keepdims=True), own_score)
    factor = jnp.exp(lse - top)
    own_weight = jnp.exp(own_score - top)
    denominator = jnp.sum(factor, -1, keepdims=True) + own_weight
    factor = factor / denominator
    own_weight = own_weight / denominator
    arrived(o_in.at[pl.ds(0, pool - 1)], 4)
    mixed = [own_weight * my_value, None, None, None]
    for s in range(pool):
        piece = factor[:, s : s + 1] * o_in[s].astype(F32)
        k = s % 4
        mixed[k] = piece if mixed[k] is None else mixed[k] + piece
    attended = ((mixed[0] + mixed[1]) + (mixed[2] + mixed[3])).astype(BF16)

    att_send[...] = attended
    for dz, dx in steps:
        send(att_send, att_all.at[me], 5, dev(at(dz, dx)))
    att_all[me] = attended
    loads[6].wait()
    arrived(att_all.at[pl.ds(0, pool - 1)], 5)
    att_rows[...] = att_all[...].astype(F32).reshape(pool * group, HD)
    for j in range(rows):
        att_lhs[:, j * HD : (j + 1) * HD] = att_rows[
            pl.ds(j, prompts, stride=rows), :
        ].astype(BF16)
    projected = jnp.dot(att_lhs[...], ow[...], preferred_element_type=F32)

    proj[0] = projected[0:half]
    proj[1] = projected[half:prompts]
    send(proj.at[1 - core], proj_in, 6, other)
    arrived(proj_in, 6)
    mid = (
        hid_cols[pl.ds(pl.multiple_of(core * half, half), half), :] + proj[core] + proj_in[...]
    ).astype(BF16)

    mid_send[...] = mid
    for dz, dx in steps:
        send(mid_send, mid_all.at[core, me], 7, dev(at(dz, dx)))
    mid_all[core, me] = mid
    arrived(mid_all.at[0, pl.ds(0, pool - 1)], 7)
    send(mid_all.at[core], mid_all.at[core], 8, other)
    arrived(mid_all.at[0], 8)

    inverse = []
    for c in range(2):
        state = mid_all[c].astype(F32)
        squares = jnp.sum(jnp.sum(state * state, 0), -1, keepdims=True)
        inverse.append(lax.rsqrt(squares * (1.0 / (pool * HD)) + EPS))
    for k in range(pool):
        chunk = jnp.concatenate([mid_all[c, k].astype(F32) * inverse[c] for c in range(2)], 0)
        normed_lhs[:, k * HD : (k + 1) * HD] = chunk.astype(BF16)
    loads[7].wait()
    loads[8].wait()
    across = (((1,), (1,)), ((), ()))
    gate = lax.dot_general(normed_lhs[...], gw[...], across, preferred_element_type=F32)
    up = lax.dot_general(normed_lhs[...], uw[...], across, preferred_element_type=F32)
    active = (gate / (1.0 + jnp.exp(-gate)) * up).astype(BF16)

    loads[9].wait()
    wide_cols = 8 * HD
    for c in range(pool // 8):
        part = jnp.dot(
            active, dw[:, c * wide_cols : (c + 1) * wide_cols], preferred_element_type=F32
        )
        for k in range(8):
            down[0, c * 8 + k] = part[0:half, k * HD : (k + 1) * HD]
            down[1, c * 8 + k] = part[half:prompts, k * HD : (k + 1) * HD]
    send(down.at[1 - core], down_in, 9, other)
    arrived(down_in, 9)
    down_send[...] = (down[core] + down_in[...]).astype(BF16)
    for dz, dx in steps:
        to = at(dz, dx)
        send(down_send.at[to], part_in.at[dz * NX + dx - 1], 10, dev(to))
    part_in[pool - 1] = down_send[me]
    arrived(part_in.at[pl.ds(0, pool - 1)], 10)
    done = mid.astype(F32) + jnp.sum(part_in[...].astype(F32), 0)
    fin[core] = done.astype(BF16)
    send(fin.at[core], fin.at[core], 11, other)
    arrived(fin.at[0], 11)
    out_ref[...] = jnp.concatenate([fin[0].astype(F32), fin[1].astype(F32)], 0).astype(BF16)

    sent(term_in, 0)
    sent(item_in, 1)
    sent(q_all.at[pl.ds(0, pool - 1)], 2)
    sent(lse_in.at[pl.ds(0, pool - 1)], 3)
    sent(o_in.at[pl.ds(0, pool - 1)], 4)
    sent(att_all.at[pl.ds(0, pool - 1)], 5)
    sent(proj_in, 6)
    sent(mid_all.at[0, pl.ds(0, pool - 1)], 7)
    sent(mid_all.at[0], 8)
    sent(down_in, 9)
    sent(part_in.at[pl.ds(0, pool - 1)], 10)
    sent(fin.at[0], 11)


def solution(mesh):
    pool = mesh.shape["pool"]

    def per_device(
        hidden_in,
        key_cache,
        value_cache,
        positions,
        query_pos,
        lengths,
        query_weight,
        key_weight,
        value_weight,
        out_weight,
        gate_weight,
        up_weight,
        down_weight,
    ):
        gate_weight, up_weight = gate_weight.T, up_weight.T
        prompts, kv, slots, _ = key_cache.shape
        group = query_weight.shape[1] // (kv * HD)
        nz = pool // NX
        parts = group + 2
        half = prompts // 2
        hbm = pl.BlockSpec(memory_space=pltpu.HBM)
        vmem = pl.BlockSpec(memory_space=pltpu.VMEM)
        smem = pl.BlockSpec(memory_space=pltpu.SMEM)

        def like(a):
            return pltpu.VMEM(a.shape, a.dtype)

        scratch = [
            like(hidden_in),
            like(key_cache),
            like(value_cache),
            like(query_weight),
            like(key_weight),
            like(value_weight),
            like(out_weight),
            like(gate_weight),
            like(up_weight),
            like(down_weight),
            pltpu.VMEM((kv, parts, prompts, HD), F32),
            pltpu.VMEM((NX - 1, parts, prompts, HD), F32),
            pltpu.VMEM((prompts, parts, HD), F32),
            pltpu.VMEM((nz - 1, parts, HD), F32),
            pltpu.VMEM((group, HD), BF16),
            pltpu.VMEM((pool, group, HD), BF16),
            pltpu.VMEM((HD, HD), F32),
            pltpu.VMEM((pool, group, HD), BF16),
            pltpu.VMEM((pool, group, HD), BF16),
            pltpu.VMEM((prompts, 1, HD), F32),
            pltpu.VMEM((pool, 1, HD), F32),
            pltpu.VMEM((HD, HD), F32),
            pltpu.VMEM((group, HD), BF16),
            pltpu.VMEM((pool, group, HD), BF16),
            pltpu.VMEM((pool * group, HD), F32),
            pltpu.VMEM((prompts, kv * group * HD), BF16),
            pltpu.VMEM((prompts, HD), F32),
            pltpu.VMEM((2, half, HD), F32),
            pltpu.VMEM((half, HD), F32),
            pltpu.VMEM((half, HD), BF16),
            pltpu.VMEM((2, pool, half, HD), BF16),
            pltpu.VMEM((prompts, pool * HD), BF16),
            pltpu.VMEM((2, pool, half, HD), F32),
            pltpu.VMEM((pool, half, HD), F32),
            pltpu.VMEM((pool, half, HD), BF16),
            pltpu.VMEM((pool, half, HD), BF16),
            pltpu.VMEM((2, half, HD), BF16),
            pltpu.SemaphoreType.DMA((10,)),
            pltpu.SemaphoreType.DMA((12,)),
            pltpu.SemaphoreType.DMA((12,)),
            pltpu.SemaphoreType.REGULAR((3,)),
        ]
        return pl.pallas_call(
            functools.partial(body, (prompts, pool, kv, group, slots)),
            out_shape=jax.ShapeDtypeStruct((prompts, HD), BF16),
            in_specs=[smem, smem, hbm, hbm, hbm, vmem] + [hbm] * 7,
            out_specs=vmem,
            scratch_shapes=scratch,
            compiler_params=pltpu.CompilerParams(
                collective_id=0, has_side_effects=True, vmem_limit_bytes=60 * 1024 * 1024
            ),
        )(
            query_pos,
            lengths,
            hidden_in,
            key_cache,
            value_cache,
            positions,
            query_weight,
            key_weight,
            value_weight,
            out_weight,
            gate_weight,
            up_weight,
            down_weight,
        )

    in_specs = (
        P("groups", None),
        P("groups", "heads", "pool", None),
        P("groups", "heads", "pool", None),
        P(None, "groups", "pool"),
        P(None, "groups"),
        P("groups"),
        P("pool", "heads"),
        P("pool", "heads"),
        P("pool", "heads"),
        P("heads", "pool"),
        P(None, ("pool", "heads")),
        P(None, ("pool", "heads")),
        P(("pool", "heads"), None),
    )
    return jax.shard_map(
        per_device, mesh=mesh, in_specs=in_specs, out_specs=P("groups", "pool"), check_vma=False
    )
```

```python
import functools
import math

import jax
import jax.numpy as jnp
from jax import lax
from jax.experimental import pallas as pl
from jax.experimental.pallas import tpu as pltpu
from jax.sharding import PartitionSpec as P

HD = 128
EPS = 1e-06
THETA = 1000000.0
NX = 4
MESH = pl.DeviceIdType.MESH
F32 = jnp.float32
BF16 = jnp.bfloat16


def far_first(pool):
    nz = pool // NX
    steps = [(a, b) for a in range(nz) for b in range(NX) if (a, b) != (0, 0)]
    return sorted(steps, key=lambda s: -(min(s[0], nz - s[0]) + min(s[1], NX - s[1])))


def rotate(values, cos_table, sin_table):
    return values * cos_table + pltpu.roll(values, HD // 2, values.ndim - 1) * sin_table


def choose_ids(lane, t, h, w):
    column = lane % (HD // 2)
    first_end = HD // 8
    second_end = first_end + 3 * HD // 16
    return jnp.where(column < first_end, t, jnp.where(column < second_end, h, w))


def inverse_row(lane):
    column = (lane % (HD // 2)).astype(F32)
    return jnp.exp(column * (-2.0 * math.log(THETA) / HD))


def body(
    cfg,
    query_pos,
    lengths,
    hidden_hbm,
    key_hbm,
    value_hbm,
    positions,
    qw_hbm,
    kw_hbm,
    vw_hbm,
    ow_hbm,
    gw_hbm,
    uw_hbm,
    dw_hbm,
    out_ref,
    hidden,
    keys,
    values,
    qw,
    kw,
    vw,
    ow,
    gw,
    uw,
    dw,
    term,
    term_in,
    item,
    item_in,
    q_send,
    q_all,
    pos_t,
    o_send,
    o_in,
    lse_send,
    lse_in,
    join,
    att_all,
    att_rows,
    att_lhs,
    hid_cols,
    proj,
    proj_in,
    mid_send,
    mid_all,
    normed_lhs,
    down,
    down_in,
    down_send,
    part_in,
    fin,
    load_sem,
    send_sem,
    recv_sem,
    here_sem,
    q_sem,
    down_sem,
):
    prompts, pool, kv, group, slots = cfg
    nz = pool // NX
    group_i = lax.axis_index("groups")
    me = lax.axis_index("pool")
    core = lax.axis_index("heads")
    z = me // NX
    x = me % NX
    half = prompts // 2
    steps = far_first(pool)

    def at(dz, dx):
        return lax.rem(z + dz, nz) * NX + lax.rem(x + dx, NX)

    def dev(p):
        return (group_i, p, core)

    other = (group_i, me, 1 - core)

    barrier = pltpu.get_barrier_semaphore()
    near = [dev(at(0, dx)) for dx in (2, 1, 3)] + [dev(at(1, 0)), dev(at(nz - 1, 0)), other]
    for device in near:
        pl.semaphore_signal(barrier, inc=1, device_id=device, device_id_type=MESH)

    def tell(distance, n):
        for dz in (distance, nz - distance):
            pl.semaphore_signal(here_sem.at[n], inc=1, device_id=dev(at(dz, 0)), device_id_type=MESH)

    loads = []
    for n, (src, dst) in enumerate(
        [
            (hidden_hbm, hidden),
            (qw_hbm, qw),
            (kw_hbm, kw),
            (vw_hbm, vw),
            (key_hbm, keys),
            (value_hbm, values),
            (ow_hbm, ow),
            (gw_hbm, gw),
            (uw_hbm, uw),
            (dw_hbm, dw),
        ]
    ):
        copy = pltpu.make_async_copy(src, dst, load_sem.at[n])
        copy.start()
        loads.append(copy)


    def send(src, dst, n, device, arrival=None):
        pltpu.make_async_remote_copy(
            src_ref=src,
            dst_ref=dst,
            send_sem=send_sem.at[n],
            recv_sem=recv_sem.at[n] if arrival is None else arrival,
            device_id=device,
            device_id_type=MESH,
        ).start()

    def arrived(view, n, arrival=None):
        pltpu.make_async_copy(view, view, recv_sem.at[n] if arrival is None else arrival).wait()

    def sent(view, n):
        pltpu.make_async_copy(view, view, send_sem.at[n]).wait()

    loads[0].wait()
    pl.semaphore_wait(barrier, len(near))
    tell(1, 0)
    wide = hidden[...].astype(F32)
    scale = lax.rsqrt(jnp.mean(wide * wide, -1, keepdims=True) + EPS)
    mine = hidden[:, pl.ds(pl.multiple_of(me * HD, HD), HD)].astype(F32)
    hid_cols[...] = mine
    normed_cols = (mine * scale).astype(BF16)
    for n in (1, 2, 3):
        loads[n].wait()
    width = group * HD
    for dx in (2, 1, 3, 0):
        g = lax.rem(x + dx, NX)
        part = jnp.dot(
            normed_cols,
            qw[:, pl.ds(pl.multiple_of(g * width, width), width)],
            preferred_element_type=F32,
        )
        for j in range(group):
            term[g, j] = part[:, j * HD : (j + 1) * HD]
        columns = pl.ds(pl.multiple_of(g * HD, HD), HD)
        term[g, group] = jnp.dot(normed_cols, kw[:, columns], preferred_element_type=F32)
        term[g, group + 1] = jnp.dot(normed_cols, vw[:, columns], preferred_element_type=F32)
        if dx:
            send(term.at[g], term_in.at[dx - 1], 0, dev(at(0, dx)))

    pl.semaphore_wait(here_sem.at[0], 2)
    tell(2, 1)
    pl.semaphore_wait(here_sem.at[1], 2)
    tell(4, 2)

    wide_pos = jnp.concatenate(
        [positions[k].astype(F32) for k in range(3)]
        + [jnp.zeros((HD - 3 * prompts, slots), F32)],
        0,
    )
    wide_pos = jnp.concatenate([wide_pos, jnp.zeros((HD, HD - slots), F32)], 1)
    pos_t[...] = wide_pos.T

    arrived(term_in, 0)
    for j in range(group + 2):
        item[:, j, :] = term[x, j] + term_in[0, j] + term_in[1, j] + term_in[2, j]

    pl.semaphore_wait(here_sem.at[2], 2)
    for dz in sorted(range(1, nz), key=lambda d: -min(d, nz - d)):
        p = lax.rem(z + dz, nz)
        send(item.at[p], item_in.at[dz - 1], 1, dev(at(dz, 0)))

    loads[4].wait()
    lane = lax.broadcasted_iota(jnp.int32, (slots, HD), 1)
    inv = inverse_row(lane)
    sign = jnp.where(lane < HD // 2, -1.0, 1.0)

    for p in range(prompts):
        ids = choose_ids(
            lane,
            pos_t[0:slots, p : p + 1],
            pos_t[0:slots, prompts + p : prompts + p + 1],
            pos_t[0:slots, 2 * prompts + p : 2 * prompts + p + 1],
        )
        angles = ids * inv
        cos_table = jnp.cos(angles)
        sin_table = jnp.sin(angles) * sign
        for g in range(kv):
            keys[p, g] = rotate(keys[p, g].astype(F32), cos_table, sin_table).astype(BF16)

    arrived(item_in, 1)
    total = item[z]
    for d in range(nz - 1):
        total = total + item_in[d]

    row = lax.broadcasted_iota(jnp.int32, (1, HD), 1)
    ids = choose_ids(
        row,
        query_pos[0, z].astype(F32),
        query_pos[1, z].astype(F32),
        query_pos[2, z].astype(F32),
    )
    angles = ids * inverse_row(row)
    cos_row = jnp.cos(angles)
    sin_row = jnp.sin(angles) * jnp.where(row < HD // 2, -1.0, 1.0)
    my_queries = rotate(total[0:group], cos_row, sin_row).astype(BF16)
    my_key = rotate(total[group : group + 1], cos_row, sin_row).astype(BF16).astype(F32)
    my_value = total[group + 1 : group + 2].astype(BF16).astype(F32)

    q_send[...] = my_queries
    for dz, dx in steps:
        send(q_send, q_all.at[me], 2, dev(at(dz, dx)), q_sem.at[dz])
    q_all[me] = my_queries
    loads[5].wait()

    rows = kv * group
    r_i = lax.broadcasted_iota(jnp.int32, (rows, kv * slots), 0)
    c_i = lax.broadcasted_iota(jnp.int32, (rows, kv * slots), 1)
    diagonal = r_i // group == c_i // slots
    slot = c_i % slots + me * slots
    lane_minus_row = lax.broadcasted_iota(jnp.int32, (rows, HD), 1) - lax.broadcasted_iota(
        jnp.int32, (rows, HD), 0
    )
    mine_here = lax.broadcasted_iota(jnp.int32, (rows, 1), 0) // group == x

    def part_of(p, own):
        first = p * kv
        q4 = q_all[pl.ds(first, kv)].astype(F32).reshape(rows, HD)
        k4 = keys[p].reshape(kv * slots, HD)
        v4 = values[p].reshape(kv * slots, HD)
        scores = lax.dot_general(
            q4.astype(BF16), k4, (((1,), (1,)), ((), ())), preferred_element_type=F32
        ) * HD ** (-0.5)
        valid = diagonal & (slot < lengths[p])
        scores = jnp.where(valid, scores, -1e30)
        peak = jnp.max(scores, -1, keepdims=True)
        if own:
            own_score = jnp.sum(q4 * my_key[0], -1, keepdims=True) * HD ** (-0.5)
            peak = jnp.where(mine_here, jnp.maximum(peak, own_score), peak)
        weights = jnp.where(valid, jnp.exp(scores - peak), 0.0).astype(BF16)
        norm = jnp.sum(weights.astype(F32), -1, keepdims=True)
        blended = jnp.dot(weights, v4, preferred_element_type=F32)
        if own:
            own_weight = jnp.where(mine_here, jnp.exp(jnp.minimum(own_score - peak, 0.0)), 0.0)
            norm = norm + own_weight
            blended = blended + own_weight * my_value[0]
        some = norm > 0.0
        safe = jnp.where(some, norm, 1.0)
        lse = jnp.where(some, peak + jnp.log(safe), -1e30)
        blended = blended / safe
        o_send[p] = blended.reshape(kv, group, HD).astype(BF16)
        eye_lse = jnp.where(lane_minus_row == 0, lse, 0.0)
        lse_send[p] = jnp.sum(eye_lse, 0, keepdims=True)

    for near in range(nz // 2 + 1):
        away = sorted({near, (nz - near) % nz})
        for dz in away:
            count = NX - 1 if dz == 0 else NX
            arrived(q_all.at[pl.ds(0, count)], 2, q_sem.at[dz])
        for dz in away:
            part_of(lax.rem(z - dz + nz, nz), dz == 0)
        for dz in away:
            p = lax.rem(z - dz + nz, nz)
            if dz != nz // 2:
                owner = dev(at(nz - dz + nz // 2, 0))
                send(lse_send.at[p], lse_in.at[z], 3, owner)
                send(o_send.at[p], o_in.at[z], 4, owner)

    theirs = lax.rem(z + nz // 2, nz)
    o_in[z] = o_send[theirs]
    lse_in[z] = lse_send[theirs]
    arrived(lse_in.at[pl.ds(0, nz - 1)], 3)
    lse_rows = jnp.concatenate(
        [lse_in[...].reshape(nz, HD), jnp.full((HD - nz, HD), -1e30, F32)], 0
    )
    lse = lse_rows.T[0:rows]
    top = jnp.max(lse, -1, keepdims=True)
    factor = jnp.exp(lse - top)
    norm = jnp.sum(factor, -1, keepdims=True)
    factor = factor / norm
    joined_lse = top + jnp.log(norm)
    arrived(o_in.at[pl.ds(0, nz - 1)], 4)
    mixed = [None, None]
    for s in range(nz):
        piece = factor[:, s : s + 1] * o_in[s].astype(F32).reshape(rows, HD)
        k = s % 2
        mixed[k] = piece if mixed[k] is None else mixed[k] + piece
    join[x, 0:kv] = (mixed[0] + mixed[1]).reshape(kv, group, HD)
    head_lane = lax.broadcasted_iota(jnp.int32, (group, HD), 1)
    packed = jnp.zeros((group, HD), F32)
    for g in range(kv):
        packed = jnp.where(head_lane == g, joined_lse[g * group : (g + 1) * group], packed)
    join[x, kv] = packed

    for dx in (2, 1, 3):
        send(join.at[x], join.at[x], 5, dev(at(0, dx)))
    arrived(join.at[pl.ds(0, NX - 1)], 5)
    attended = []
    for g in range(kv):
        lse = [join[n, kv][:, g : g + 1] for n in range(NX)]
        top = jnp.maximum(jnp.maximum(lse[0], lse[1]), jnp.maximum(lse[2], lse[3]))
        factor = [jnp.exp(v - top) for v in lse]
        norm = (factor[0] + factor[1]) + (factor[2] + factor[3])
        total = sum(factor[n] * join[n, g] for n in range(NX)) / norm
        attended.append(total.astype(BF16))

    for g in range(kv):
        att_all[theirs, g] = attended[g]
    for dz in sorted(range(1, nz), key=lambda d: -min(d, nz - d)):
        send(att_all.at[theirs], att_all.at[theirs], 12, dev(at(dz, 0)))
    loads[6].wait()
    arrived(att_all.at[pl.ds(0, nz - 1)], 12)
    att_rows[...] = att_all[...].astype(F32).reshape(pool * group, HD)
    for j in range(rows):
        att_lhs[:, j * HD : (j + 1) * HD] = att_rows[
            pl.ds(j, prompts, stride=rows), :
        ].astype(BF16)
    projected = jnp.dot(att_lhs[...], ow[...], preferred_element_type=F32)

    proj[0] = projected[0:half]
    proj[1] = projected[half:prompts]
    send(proj.at[1 - core], proj_in, 6, other)
    arrived(proj_in, 6)
    mid = (
        hid_cols[pl.ds(pl.multiple_of(core * half, half), half), :] + proj[core] + proj_in[...]
    ).astype(BF16)

    mid_send[...] = mid
    for dz, dx in steps:
        send(mid_send, mid_all.at[core, me], 7, dev(at(dz, dx)))
    mid_all[core, me] = mid
    arrived(mid_all.at[0, pl.ds(0, pool - 1)], 7)
    send(mid_all.at[core], mid_all.at[core], 8, other)
    arrived(mid_all.at[0], 8)

    inverse = []
    for c in range(2):
        state = mid_all[c].astype(F32)
        squares = jnp.sum(jnp.sum(state * state, 0), -1, keepdims=True)
        inverse.append(lax.rsqrt(squares * (1.0 / (pool * HD)) + EPS))
    for k in range(pool):
        chunk = jnp.concatenate([mid_all[c, k].astype(F32) * inverse[c] for c in range(2)], 0)
        normed_lhs[:, k * HD : (k + 1) * HD] = chunk.astype(BF16)
    loads[7].wait()
    loads[8].wait()
    across = (((1,), (1,)), ((), ()))
    gate = lax.dot_general(normed_lhs[...], gw[...], across, preferred_element_type=F32)
    up = lax.dot_general(normed_lhs[...], uw[...], across, preferred_element_type=F32)
    active = (gate / (1.0 + jnp.exp(-gate)) * up).astype(BF16)

    loads[9].wait()
    order = sorted(range(nz), key=lambda d: -min(d, nz - d))

    def down_columns(n):
        for dz in order[n * NX : (n + 1) * NX]:
            first = lax.rem(z + dz, nz) * NX
            part = jnp.dot(
                active,
                dw[:, pl.ds(pl.multiple_of(first * HD, NX * HD), NX * HD)],
                preferred_element_type=F32,
            )
            at_n = (n * NX + order[n * NX : (n + 1) * NX].index(dz)) * NX
            for k in range(NX):
                down[0, at_n + k] = part[0:half, k * HD : (k + 1) * HD]
                down[1, at_n + k] = part[half:prompts, k * HD : (k + 1) * HD]
        block = pl.ds(n * NX * NX, NX * NX)
        send(down.at[1 - core, block], down_in.at[block], 9, other, down_sem.at[n])

    def down_out(n):
        block = pl.ds(n * NX * NX, NX * NX)
        arrived(down_in.at[block], 9, down_sem.at[n])
        down_send[block] = (down[core, block] + down_in[block]).astype(BF16)
        for i, dz in enumerate(order[n * NX : (n + 1) * NX]):
            for dx in (2, 1, 3, 0):
                if dz == 0 and dx == 0:
                    continue
                entry = (n * NX + i) * NX + lax.rem(x + dx, NX)
                send(down_send.at[entry], part_in.at[dz * NX + dx - 1], 10, dev(at(dz, dx)))

    down_columns(0)
    down_columns(1)
    for n in range(2, nz // NX):
        down_out(n - 2)
        down_columns(n)
    down_out(nz // NX - 2)
    down_out(nz // NX - 1)
    part_in[pool - 1] = down_send[(nz - 1) * NX + x]
    arrived(part_in.at[pl.ds(0, pool - 1)], 10)
    done = mid.astype(F32) + jnp.sum(part_in[...].astype(F32), 0)
    fin[core] = done.astype(BF16)
    send(fin.at[core], fin.at[core], 11, other)
    arrived(fin.at[0], 11)
    out_ref[...] = jnp.concatenate([fin[0].astype(F32), fin[1].astype(F32)], 0).astype(BF16)

    sent(term_in, 0)
    sent(item_in, 1)
    sent(q_all.at[pl.ds(0, pool - 1)], 2)
    sent(lse_in.at[pl.ds(0, nz - 1)], 3)
    sent(o_in.at[pl.ds(0, nz - 1)], 4)
    sent(join.at[pl.ds(0, NX - 1)], 5)
    sent(att_all.at[pl.ds(0, nz - 1)], 12)
    sent(proj_in, 6)
    sent(mid_all.at[0, pl.ds(0, pool - 1)], 7)
    sent(mid_all.at[0], 8)
    sent(down_in, 9)
    sent(part_in.at[pl.ds(0, pool - 1)], 10)
    sent(fin.at[0], 11)


def solution(mesh):
    pool = mesh.shape["pool"]

    def per_device(
        hidden_in,
        key_cache,
        value_cache,
        positions,
        query_pos,
        lengths,
        query_weight,
        key_weight,
        value_weight,
        out_weight,
        gate_weight,
        up_weight,
        down_weight,
    ):
        gate_weight, up_weight = gate_weight.T, up_weight.T
        prompts, kv, slots, _ = key_cache.shape
        group = query_weight.shape[1] // (kv * HD)
        nz = pool // NX
        parts = group + 2
        half = prompts // 2
        hbm = pl.BlockSpec(memory_space=pltpu.HBM)
        vmem = pl.BlockSpec(memory_space=pltpu.VMEM)
        smem = pl.BlockSpec(memory_space=pltpu.SMEM)

        def like(a):
            return pltpu.VMEM(a.shape, a.dtype)

        scratch = [
            like(hidden_in),
            like(key_cache),
            like(value_cache),
            like(query_weight),
            like(key_weight),
            like(value_weight),
            like(out_weight),
            like(gate_weight),
            like(up_weight),
            like(down_weight),
            pltpu.VMEM((kv, parts, prompts, HD), F32),
            pltpu.VMEM((NX - 1, parts, prompts, HD), F32),
            pltpu.VMEM((prompts, parts, HD), F32),
            pltpu.VMEM((nz - 1, parts, HD), F32),
            pltpu.VMEM((group, HD), BF16),
            pltpu.VMEM((pool, group, HD), BF16),
            pltpu.VMEM((HD, HD), F32),
            pltpu.VMEM((prompts, kv, group, HD), BF16),
            pltpu.VMEM((nz, kv, group, HD), BF16),
            pltpu.VMEM((prompts, 1, HD), F32),
            pltpu.VMEM((nz, 1, HD), F32),
            pltpu.VMEM((NX, kv + 1, group, HD), F32),
            pltpu.VMEM((prompts, kv, group, HD), BF16),
            pltpu.VMEM((pool * group, HD), F32),
            pltpu.VMEM((prompts, kv * group * HD), BF16),
            pltpu.VMEM((prompts, HD), F32),
            pltpu.VMEM((2, half, HD), F32),
            pltpu.VMEM((half, HD), F32),
            pltpu.VMEM((half, HD), BF16),
            pltpu.VMEM((2, pool, half, HD), BF16),
            pltpu.VMEM((prompts, pool * HD), BF16),
            pltpu.VMEM((2, pool, half, HD), F32),
            pltpu.VMEM((pool, half, HD), F32),
            pltpu.VMEM((pool, half, HD), BF16),
            pltpu.VMEM((pool, half, HD), BF16),
            pltpu.VMEM((2, half, HD), BF16),
            pltpu.SemaphoreType.DMA((10,)),
            pltpu.SemaphoreType.DMA((13,)),
            pltpu.SemaphoreType.DMA((13,)),
            pltpu.SemaphoreType.REGULAR((3,)),
            pltpu.SemaphoreType.DMA((nz,)),
            pltpu.SemaphoreType.DMA((nz // NX,)),
        ]
        return pl.pallas_call(
            functools.partial(body, (prompts, pool, kv, group, slots)),
            out_shape=jax.ShapeDtypeStruct((prompts, HD), BF16),
            in_specs=[smem, smem, hbm, hbm, hbm, vmem] + [hbm] * 7,
            out_specs=vmem,
            scratch_shapes=scratch,
            compiler_params=pltpu.CompilerParams(
                collective_id=0, has_side_effects=True, vmem_limit_bytes=60 * 1024 * 1024
            ),
        )(
            query_pos,
            lengths,
            hidden_in,
            key_cache,
            value_cache,
            positions,
            query_weight,
            key_weight,
            value_weight,
            out_weight,
            gate_weight,
            up_weight,
            down_weight,
        )

    in_specs = (
        P("groups", None),
        P("groups", "heads", "pool", None),
        P("groups", "heads", "pool", None),
        P(None, "groups", "pool"),
        P(None, "groups"),
        P("groups"),
        P("pool", "heads"),
        P("pool", "heads"),
        P("pool", "heads"),
        P("heads", "pool"),
        P(None, ("pool", "heads")),
        P(None, ("pool", "heads")),
        P(("pool", "heads"), None),
    )
    return jax.shard_map(
        per_device, mesh=mesh, in_specs=in_specs, out_specs=P("groups", "pool"), check_vma=False
    )
```

```python
import functools
import math

import jax
import jax.numpy as jnp
from jax import lax
from jax.experimental import pallas as pl
from jax.experimental.pallas import tpu as pltpu
from jax.sharding import PartitionSpec as P

HD = 128
EPS = 1e-06
THETA = 1000000.0
LAG = 6
NX = 4
MESH = pl.DeviceIdType.MESH
F32 = jnp.float32
BF16 = jnp.bfloat16


def far_first(pool):
    nz = pool // NX
    steps = [(a, b) for a in range(nz) for b in range(NX) if (a, b) != (0, 0)]
    return sorted(steps, key=lambda s: -(min(s[0], nz - s[0]) + min(s[1], NX - s[1])))


def rotate(values, cos_table, sin_table):
    return values * cos_table + pltpu.roll(values, HD // 2, values.ndim - 1) * sin_table


def choose_ids(lane, t, h, w):
    column = lane % (HD // 2)
    first_end = HD // 8
    second_end = first_end + 3 * HD // 16
    return jnp.where(column < first_end, t, jnp.where(column < second_end, h, w))


def inverse_row(lane):
    column = (lane % (HD // 2)).astype(F32)
    return jnp.exp(column * (-2.0 * math.log(THETA) / HD))


def body(
    cfg,
    query_pos_hbm,
    lengths_hbm,
    hidden_hbm,
    key_hbm,
    value_hbm,
    positions_hbm,
    qw_hbm,
    kw_hbm,
    vw_hbm,
    ow_hbm,
    gw_hbm,
    uw_hbm,
    dw_hbm,
    out_ref,
    query_pos,
    lengths,
    positions,
    hidden,
    keys,
    values,
    qw,
    kw,
    vw,
    ow,
    gw,
    uw,
    dw,
    term,
    term_in,
    item,
    item_in,
    q_send,
    q_all,
    pos_t,
    o_send,
    o_in,
    lse_send,
    lse_in,
    join,
    att_all,
    att_rows,
    att_lhs,
    hid_cols,
    proj,
    proj_in,
    mid_send,
    mid_all,
    normed_lhs,
    down,
    down_in,
    down_send,
    part_in,
    fin,
    load_sem,
    send_sem,
    recv_sem,
    here_sem,
    q_sem,
    down_sem,
    q_x_sem,
):
    prompts, pool, kv, group, slots = cfg
    nz = pool // NX
    group_i = lax.axis_index("groups")
    me = lax.axis_index("pool")
    core = lax.axis_index("heads")
    z = me // NX
    x = me % NX
    half = prompts // 2
    steps = far_first(pool)

    def at(dz, dx):
        return lax.rem(z + dz, nz) * NX + lax.rem(x + dx, NX)

    def dev(p):
        return (group_i, p, core)

    other = (group_i, me, 1 - core)

    loads = []
    for n, (src, dst) in enumerate(
        [
            (hidden_hbm, hidden),
            (qw_hbm, qw),
            (kw_hbm, kw),
            (vw_hbm, vw),
            (key_hbm, keys),
            (value_hbm, values),
            (ow_hbm, ow),
            (gw_hbm, gw),
            (uw_hbm, uw),
            (dw_hbm, dw),
            (positions_hbm, positions),
            (query_pos_hbm, query_pos),
            (lengths_hbm, lengths),
        ]
    ):
        copy = pltpu.make_async_copy(src, dst, load_sem.at[n])
        loads.append(copy)
    for n in (0, 1, 2, 3):
        loads[n].start()


    barrier = pltpu.get_barrier_semaphore()
    near = [dev(at(0, dx)) for dx in (2, 1, 3)] + [dev(at(1, 0)), dev(at(nz - 1, 0)), other]
    for device in near:
        pl.semaphore_signal(barrier, inc=1, device_id=device, device_id_type=MESH)

    def tell(distance, n):
        for dz in (distance, nz - distance):
            pl.semaphore_signal(here_sem.at[n], inc=1, device_id=dev(at(dz, 0)), device_id_type=MESH)

    for n in (10, 11, 12, 4, 5, 6, 7, 8, 9):
        loads[n].start()

    def send(src, dst, n, device, arrival=None):
        pltpu.make_async_remote_copy(
            src_ref=src,
            dst_ref=dst,
            send_sem=send_sem.at[n],
            recv_sem=recv_sem.at[n] if arrival is None else arrival,
            device_id=device,
            device_id_type=MESH,
        ).start()

    def arrived(view, n, arrival=None):
        pltpu.make_async_copy(view, view, recv_sem.at[n] if arrival is None else arrival).wait()

    def sent(view, n):
        pltpu.make_async_copy(view, view, send_sem.at[n]).wait()

    loads[0].wait()
    pl.semaphore_wait(barrier, len(near))
    tell(1, 0)
    wide = hidden[...].astype(F32)
    scale = lax.rsqrt(jnp.mean(wide * wide, -1, keepdims=True) + EPS)
    mine = hidden[:, pl.ds(pl.multiple_of(me * HD, HD), HD)].astype(F32)
    hid_cols[...] = mine
    normed_cols = (mine * scale).astype(BF16)
    for n in (1, 2, 3):
        loads[n].wait()
    width = group * HD
    for dx in (2, 1, 3, 0):
        g = lax.rem(x + dx, NX)
        part = jnp.dot(
            normed_cols,
            qw[:, pl.ds(pl.multiple_of(g * width, width), width)],
            preferred_element_type=F32,
        )
        for j in range(group):
            term[g, j] = part[:, j * HD : (j + 1) * HD]
        columns = pl.ds(pl.multiple_of(g * HD, HD), HD)
        term[g, group] = jnp.dot(normed_cols, kw[:, columns], preferred_element_type=F32)
        term[g, group + 1] = jnp.dot(normed_cols, vw[:, columns], preferred_element_type=F32)
        if dx:
            send(term.at[g], term_in.at[dx - 1], 0, dev(at(0, dx)))

    pl.semaphore_wait(here_sem.at[0], 2)
    tell(2, 1)
    pl.semaphore_wait(here_sem.at[1], 2)
    tell(4, 2)

    for n in (10, 11, 12):
        loads[n].wait()
    wide_pos = jnp.concatenate(
        [positions[k].astype(F32) for k in range(3)]
        + [jnp.zeros((HD - 3 * prompts, slots), F32)],
        0,
    )
    wide_pos = jnp.concatenate([wide_pos, jnp.zeros((HD, HD - slots), F32)], 1)
    pos_t[...] = wide_pos.T

    arrived(term_in, 0)
    for j in range(group + 2):
        item[:, j, :] = term[x, j] + term_in[0, j] + term_in[1, j] + term_in[2, j]

    pl.semaphore_wait(here_sem.at[2], 2)
    for dz in sorted(range(1, nz), key=lambda d: -min(d, nz - d)):
        p = lax.rem(z + dz, nz)
        send(item.at[p], item_in.at[dz - 1], 1, dev(at(dz, 0)))

    loads[4].wait()
    lane = lax.broadcasted_iota(jnp.int32, (slots, HD), 1)
    inv = inverse_row(lane)
    sign = jnp.where(lane < HD // 2, -1.0, 1.0)

    for p in range(prompts):
        ids = choose_ids(
            lane,
            pos_t[0:slots, p : p + 1],
            pos_t[0:slots, prompts + p : prompts + p + 1],
            pos_t[0:slots, 2 * prompts + p : 2 * prompts + p + 1],
        )
        angles = ids * inv
        cos_table = jnp.cos(angles)
        sin_table = jnp.sin(angles) * sign
        for g in range(kv):
            keys[p, g] = rotate(keys[p, g].astype(F32), cos_table, sin_table).astype(BF16)

    arrived(item_in, 1)
    total = item[z]
    for d in range(nz - 1):
        total = total + item_in[d]

    row = lax.broadcasted_iota(jnp.int32, (1, HD), 1)
    ids = choose_ids(
        row,
        query_pos[0, z].astype(F32),
        query_pos[1, z].astype(F32),
        query_pos[2, z].astype(F32),
    )
    angles = ids * inverse_row(row)
    cos_row = jnp.cos(angles)
    sin_row = jnp.sin(angles) * jnp.where(row < HD // 2, -1.0, 1.0)
    my_queries = rotate(total[0:group], cos_row, sin_row).astype(BF16)
    my_key = rotate(total[group : group + 1], cos_row, sin_row).astype(BF16).astype(F32)
    my_value = total[group + 1 : group + 2].astype(BF16).astype(F32)

    q_send[...] = my_queries
    q_all[me] = my_queries
    for dz in sorted(range(1, nz), key=lambda d: -min(d, nz - d)):
        send(q_send, q_all.at[me], 2, dev(at(dz, 0)), q_sem.at[dz])
    loads[5].wait()

    rows = kv * group
    r_i = lax.broadcasted_iota(jnp.int32, (rows, kv * slots), 0)
    c_i = lax.broadcasted_iota(jnp.int32, (rows, kv * slots), 1)
    diagonal = r_i // group == c_i // slots
    slot = c_i % slots + me * slots
    lane_minus_row = lax.broadcasted_iota(jnp.int32, (rows, HD), 1) - lax.broadcasted_iota(
        jnp.int32, (rows, HD), 0
    )
    mine_here = lax.broadcasted_iota(jnp.int32, (rows, 1), 0) // group == x

    def part_of(p, own):
        first = p * kv
        q4 = q_all[pl.ds(first, kv)].astype(F32).reshape(rows, HD)
        k4 = keys[p].reshape(kv * slots, HD)
        v4 = values[p].reshape(kv * slots, HD)
        scores = lax.dot_general(
            q4.astype(BF16), k4, (((1,), (1,)), ((), ())), preferred_element_type=F32
        ) * HD ** (-0.5)
        valid = diagonal & (slot < lengths[p])
        scores = jnp.where(valid, scores, -1e30)
        peak = jnp.max(scores, -1, keepdims=True)
        if own:
            own_score = jnp.sum(q4 * my_key[0], -1, keepdims=True) * HD ** (-0.5)
            peak = jnp.where(mine_here, jnp.maximum(peak, own_score), peak)
        weights = jnp.where(valid, jnp.exp(scores - peak), 0.0).astype(BF16)
        norm = jnp.sum(weights.astype(F32), -1, keepdims=True)
        blended = jnp.dot(weights, v4, preferred_element_type=F32)
        if own:
            own_weight = jnp.where(mine_here, jnp.exp(jnp.minimum(own_score - peak, 0.0)), 0.0)
            norm = norm + own_weight
            blended = blended + own_weight * my_value[0]
        some = norm > 0.0
        safe = jnp.where(some, norm, 1.0)
        lse = jnp.where(some, peak + jnp.log(safe), -1e30)
        blended = blended / safe
        o_send[p] = blended.reshape(kv, group, HD).astype(BF16)
        eye_lse = jnp.where(lane_minus_row == 0, lse, 0.0)
        lse_send[p] = jnp.sum(eye_lse, 0, keepdims=True)

    def away_at(near):
        return sorted({near, (nz - near) % nz})

    def relay(near):
        for dz in away_at(near):
            entry = lax.rem(z - dz + nz, nz) * kv + x
            if dz:
                arrived(q_all.at[pl.ds(0, 1)], 2, q_sem.at[dz])
            for dx in (2, 1, 3):
                send(q_all.at[entry], q_all.at[entry], 13, dev(at(0, dx)), q_x_sem.at[dz])

    def attend(near):
        away = away_at(near)
        for dz in away:
            arrived(q_all.at[pl.ds(0, NX - 1)], 13, q_x_sem.at[dz])
        for dz in away:
            part_of(lax.rem(z - dz + nz, nz), dz == 0)
        for dz in away:
            p = lax.rem(z - dz + nz, nz)
            if dz != nz // 2:
                owner = dev(at(nz - dz + nz // 2, 0))
                send(lse_send.at[p], lse_in.at[z], 3, owner)
                send(o_send.at[p], o_in.at[z], 4, owner)

    reach = nz // 2 + 1
    for near in range(reach + LAG):
        if near < reach:
            relay(near)
        if near >= LAG:
            attend(near - LAG)

    theirs = lax.rem(z + nz // 2, nz)
    o_in[z] = o_send[theirs]
    lse_in[z] = lse_send[theirs]
    arrived(lse_in.at[pl.ds(0, nz - 1)], 3)
    lse_rows = jnp.concatenate(
        [lse_in[...].reshape(nz, HD), jnp.full((HD - nz, HD), -1e30, F32)], 0
    )
    lse = lse_rows.T[0:rows]
    top = jnp.max(lse, -1, keepdims=True)
    factor = jnp.exp(lse - top)
    norm = jnp.sum(factor, -1, keepdims=True)
    factor = factor / norm
    joined_lse = top + jnp.log(norm)
    arrived(o_in.at[pl.ds(0, nz - 1)], 4)
    mixed = [None, None]
    for s in range(nz):
        piece = factor[:, s : s + 1] * o_in[s].astype(F32).reshape(rows, HD)
        k = s % 2
        mixed[k] = piece if mixed[k] is None else mixed[k] + piece
    join[x, 0:kv] = (mixed[0] + mixed[1]).reshape(kv, group, HD)
    head_lane = lax.broadcasted_iota(jnp.int32, (group, HD), 1)
    packed = jnp.zeros((group, HD), F32)
    for g in range(kv):
        packed = jnp.where(head_lane == g, joined_lse[g * group : (g + 1) * group], packed)
    join[x, kv] = packed

    for dx in (2, 1, 3):
        send(join.at[x], join.at[x], 5, dev(at(0, dx)))
    arrived(join.at[pl.ds(0, NX - 1)], 5)
    attended = []
    for g in range(kv):
        lse = [join[n, kv][:, g : g + 1] for n in range(NX)]
        top = jnp.maximum(jnp.maximum(lse[0], lse[1]), jnp.maximum(lse[2], lse[3]))
        factor = [jnp.exp(v - top) for v in lse]
        norm = (factor[0] + factor[1]) + (factor[2] + factor[3])
        total = sum(factor[n] * join[n, g] for n in range(NX)) / norm
        attended.append(total.astype(BF16))

    for g in range(kv):
        att_all[theirs, g] = attended[g]
    for dz in sorted(range(1, nz), key=lambda d: -min(d, nz - d)):
        send(att_all.at[theirs], att_all.at[theirs], 12, dev(at(dz, 0)))
    loads[6].wait()
    arrived(att_all.at[pl.ds(0, nz - 1)], 12)
    att_rows[...] = att_all[...].astype(F32).reshape(pool * group, HD)
    for j in range(rows):
        att_lhs[:, j * HD : (j + 1) * HD] = att_rows[
            pl.ds(j, prompts, stride=rows), :
        ].astype(BF16)
    projected = jnp.dot(att_lhs[...], ow[...], preferred_element_type=F32)

    proj[0] = projected[0:half]
    proj[1] = projected[half:prompts]
    send(proj.at[1 - core], proj_in, 6, other)
    arrived(proj_in, 6)
    mid = (
        hid_cols[pl.ds(pl.multiple_of(core * half, half), half), :] + proj[core] + proj_in[...]
    ).astype(BF16)

    mid_send[...] = mid
    for dz, dx in steps:
        send(mid_send, mid_all.at[core, me], 7, dev(at(dz, dx)))
    mid_all[core, me] = mid
    arrived(mid_all.at[0, pl.ds(0, pool - 1)], 7)
    send(mid_all.at[core], mid_all.at[core], 8, other)
    arrived(mid_all.at[0], 8)

    inverse = []
    for c in range(2):
        state = mid_all[c].astype(F32)
        squares = jnp.sum(jnp.sum(state * state, 0), -1, keepdims=True)
        inverse.append(lax.rsqrt(squares * (1.0 / (pool * HD)) + EPS))
    for k in range(pool):
        chunk = jnp.concatenate([mid_all[c, k].astype(F32) * inverse[c] for c in range(2)], 0)
        normed_lhs[:, k * HD : (k + 1) * HD] = chunk.astype(BF16)
    loads[7].wait()
    loads[8].wait()
    across = (((1,), (1,)), ((), ()))
    gate = lax.dot_general(normed_lhs[...], gw[...], across, preferred_element_type=F32)
    up = lax.dot_general(normed_lhs[...], uw[...], across, preferred_element_type=F32)
    active = (gate / (1.0 + jnp.exp(-gate)) * up).astype(BF16)

    loads[9].wait()
    order = sorted(range(nz), key=lambda d: -min(d, nz - d))

    def down_columns(n):
        for dz in order[n * NX : (n + 1) * NX]:
            first = lax.rem(z + dz, nz) * NX
            part = jnp.dot(
                active,
                dw[:, pl.ds(pl.multiple_of(first * HD, NX * HD), NX * HD)],
                preferred_element_type=F32,
            )
            at_n = (n * NX + order[n * NX : (n + 1) * NX].index(dz)) * NX
            for k in range(NX):
                down[0, at_n + k] = part[0:half, k * HD : (k + 1) * HD]
                down[1, at_n + k] = part[half:prompts, k * HD : (k + 1) * HD]
        block = pl.ds(n * NX * NX, NX * NX)
        send(down.at[1 - core, block], down_in.at[block], 9, other, down_sem.at[n])

    def down_out(n):
        block = pl.ds(n * NX * NX, NX * NX)
        arrived(down_in.at[block], 9, down_sem.at[n])
        down_send[block] = (down[core, block] + down_in[block]).astype(BF16)
        for i, dz in enumerate(order[n * NX : (n + 1) * NX]):
            for dx in (2, 1, 3, 0):
                if dz == 0 and dx == 0:
                    continue
                entry = (n * NX + i) * NX + lax.rem(x + dx, NX)
                send(down_send.at[entry], part_in.at[dz * NX + dx - 1], 10, dev(at(dz, dx)))

    down_columns(0)
    down_columns(1)
    for n in range(2, nz // NX):
        down_out(n - 2)
        down_columns(n)
    down_out(nz // NX - 2)
    down_out(nz // NX - 1)
    part_in[pool - 1] = down_send[(nz - 1) * NX + x]
    arrived(part_in.at[pl.ds(0, pool - 1)], 10)
    done = mid.astype(F32) + jnp.sum(part_in[...].astype(F32), 0)
    fin[core] = done.astype(BF16)
    send(fin.at[core], fin.at[core], 11, other)
    arrived(fin.at[0], 11)
    out_ref[...] = jnp.concatenate([fin[0].astype(F32), fin[1].astype(F32)], 0).astype(BF16)

    sent(term_in, 0)
    sent(item_in, 1)
    sent(q_all.at[pl.ds(0, nz - 1)], 2)
    sent(q_all.at[pl.ds(0, nz * (NX - 1))], 13)
    sent(lse_in.at[pl.ds(0, nz - 1)], 3)
    sent(o_in.at[pl.ds(0, nz - 1)], 4)
    sent(join.at[pl.ds(0, NX - 1)], 5)
    sent(att_all.at[pl.ds(0, nz - 1)], 12)
    sent(proj_in, 6)
    sent(mid_all.at[0, pl.ds(0, pool - 1)], 7)
    sent(mid_all.at[0], 8)
    sent(down_in, 9)
    sent(part_in.at[pl.ds(0, pool - 1)], 10)
    sent(fin.at[0], 11)


def solution(mesh):
    pool = mesh.shape["pool"]

    def per_device(
        hidden_in,
        key_cache,
        value_cache,
        positions,
        query_pos,
        lengths,
        query_weight,
        key_weight,
        value_weight,
        out_weight,
        gate_weight,
        up_weight,
        down_weight,
    ):
        gate_weight, up_weight = gate_weight.T, up_weight.T
        prompts, kv, slots, _ = key_cache.shape
        group = query_weight.shape[1] // (kv * HD)
        nz = pool // NX
        parts = group + 2
        half = prompts // 2
        hbm = pl.BlockSpec(memory_space=pltpu.HBM)
        vmem = pl.BlockSpec(memory_space=pltpu.VMEM)

        def like(a):
            return pltpu.VMEM(a.shape, a.dtype)

        scratch = [
            pltpu.SMEM(query_pos.shape, jnp.int32),
            pltpu.SMEM(lengths.shape, jnp.int32),
            like(positions),
            like(hidden_in),
            like(key_cache),
            like(value_cache),
            like(query_weight),
            like(key_weight),
            like(value_weight),
            like(out_weight),
            like(gate_weight),
            like(up_weight),
            like(down_weight),
            pltpu.VMEM((kv, parts, prompts, HD), F32),
            pltpu.VMEM((NX - 1, parts, prompts, HD), F32),
            pltpu.VMEM((prompts, parts, HD), F32),
            pltpu.VMEM((nz - 1, parts, HD), F32),
            pltpu.VMEM((group, HD), BF16),
            pltpu.VMEM((pool, group, HD), BF16),
            pltpu.VMEM((HD, HD), F32),
            pltpu.VMEM((prompts, kv, group, HD), BF16),
            pltpu.VMEM((nz, kv, group, HD), BF16),
            pltpu.VMEM((prompts, 1, HD), F32),
            pltpu.VMEM((nz, 1, HD), F32),
            pltpu.VMEM((NX, kv + 1, group, HD), F32),
            pltpu.VMEM((prompts, kv, group, HD), BF16),
            pltpu.VMEM((pool * group, HD), F32),
            pltpu.VMEM((prompts, kv * group * HD), BF16),
            pltpu.VMEM((prompts, HD), F32),
            pltpu.VMEM((2, half, HD), F32),
            pltpu.VMEM((half, HD), F32),
            pltpu.VMEM((half, HD), BF16),
            pltpu.VMEM((2, pool, half, HD), BF16),
            pltpu.VMEM((prompts, pool * HD), BF16),
            pltpu.VMEM((2, pool, half, HD), F32),
            pltpu.VMEM((pool, half, HD), F32),
            pltpu.VMEM((pool, half, HD), BF16),
            pltpu.VMEM((pool, half, HD), BF16),
            pltpu.VMEM((2, half, HD), BF16),
            pltpu.SemaphoreType.DMA((13,)),
            pltpu.SemaphoreType.DMA((14,)),
            pltpu.SemaphoreType.DMA((14,)),
            pltpu.SemaphoreType.REGULAR((3,)),
            pltpu.SemaphoreType.DMA((nz,)),
            pltpu.SemaphoreType.DMA((nz // NX,)),
            pltpu.SemaphoreType.DMA((nz,)),
        ]
        return pl.pallas_call(
            functools.partial(body, (prompts, pool, kv, group, slots)),
            out_shape=jax.ShapeDtypeStruct((prompts, HD), BF16),
            in_specs=[hbm] * 13,
            out_specs=vmem,
            scratch_shapes=scratch,
            compiler_params=pltpu.CompilerParams(
                collective_id=0, has_side_effects=True, vmem_limit_bytes=60 * 1024 * 1024
            ),
        )(
            query_pos,
            lengths,
            hidden_in,
            key_cache,
            value_cache,
            positions,
            query_weight,
            key_weight,
            value_weight,
            out_weight,
            gate_weight,
            up_weight,
            down_weight,
        )

    in_specs = (
        P("groups", None),
        P("groups", "heads", "pool", None),
        P("groups", "heads", "pool", None),
        P(None, "groups", "pool"),
        P(None, "groups"),
        P("groups"),
        P("pool", "heads"),
        P("pool", "heads"),
        P("pool", "heads"),
        P("heads", "pool"),
        P(None, ("pool", "heads")),
        P(None, ("pool", "heads")),
        P(("pool", "heads"), None),
    )
    return jax.shard_map(
        per_device, mesh=mesh, in_specs=in_specs, out_specs=P("groups", "pool"), check_vma=False
    )
```

```python
import functools
import math

import jax
import jax.numpy as jnp
from jax import lax
from jax.experimental import pallas as pl
from jax.experimental.pallas import tpu as pltpu
from jax.sharding import PartitionSpec as P

HD = 128
EPS = 1e-06
THETA = 1000000.0
LAG = 6
NX = 4
MESH = pl.DeviceIdType.MESH
F32 = jnp.float32
BF16 = jnp.bfloat16


def far_first(pool):
    nz = pool // NX
    steps = [(a, b) for a in range(nz) for b in range(NX) if (a, b) != (0, 0)]
    return sorted(steps, key=lambda s: -(min(s[0], nz - s[0]) + min(s[1], NX - s[1])))


def rotate(values, cos_table, sin_table):
    return values * cos_table + pltpu.roll(values, HD // 2, values.ndim - 1) * sin_table


def choose_ids(lane, t, h, w):
    column = lane % (HD // 2)
    first_end = HD // 8
    second_end = first_end + 3 * HD // 16
    return jnp.where(column < first_end, t, jnp.where(column < second_end, h, w))


def inverse_row(lane):
    column = (lane % (HD // 2)).astype(F32)
    return jnp.exp(column * (-2.0 * math.log(THETA) / HD))


def body(
    cfg,
    query_pos_hbm,
    lengths_hbm,
    hidden_hbm,
    key_hbm,
    value_hbm,
    positions_hbm,
    qw_hbm,
    kw_hbm,
    vw_hbm,
    ow_hbm,
    gw_hbm,
    uw_hbm,
    dw_hbm,
    out_ref,
    query_pos,
    lengths,
    positions,
    hidden,
    keys,
    values,
    qw,
    kw,
    vw,
    ow,
    gw,
    uw,
    dw,
    term,
    term_in,
    item,
    item_in,
    q_send,
    q_all,
    pos_t,
    o_send,
    o_in,
    lse_send,
    lse_in,
    join,
    att_all,
    att_rows,
    att_lhs,
    hid_cols,
    proj,
    proj_in,
    mid_send,
    mid_all,
    normed_lhs,
    down,
    down_in,
    down_send,
    part_in,
    fin,
    load_sem,
    send_sem,
    recv_sem,
    here_sem,
    q_sem,
    down_sem,
    q_x_sem,
):
    prompts, pool, kv, group, slots = cfg
    nz = pool // NX
    group_i = lax.axis_index("groups")
    me = lax.axis_index("pool")
    core = lax.axis_index("heads")
    z = me // NX
    x = me % NX
    half = prompts // 2
    steps = far_first(pool)

    def at(dz, dx):
        return lax.rem(z + dz, nz) * NX + lax.rem(x + dx, NX)

    def dev(p):
        return (group_i, p, core)

    other = (group_i, me, 1 - core)

    loads = []
    for n, (src, dst) in enumerate(
        [
            (hidden_hbm, hidden),
            (qw_hbm, qw),
            (kw_hbm, kw),
            (vw_hbm, vw),
            (key_hbm, keys),
            (value_hbm, values),
            (ow_hbm, ow),
            (gw_hbm, gw),
            (uw_hbm, uw),
            (dw_hbm, dw),
            (positions_hbm, positions),
            (query_pos_hbm, query_pos),
            (lengths_hbm, lengths),
        ]
    ):
        copy = pltpu.make_async_copy(src, dst, load_sem.at[n])
        loads.append(copy)
    for n in (0, 1, 2, 3):
        loads[n].start()


    barrier = pltpu.get_barrier_semaphore()
    near = [dev(at(0, dx)) for dx in (2, 1, 3)] + [dev(at(1, 0)), dev(at(nz - 1, 0)), other]
    for device in near:
        pl.semaphore_signal(barrier, inc=1, device_id=device, device_id_type=MESH)

    def tell(distance, n):
        for dz in (distance, nz - distance):
            pl.semaphore_signal(here_sem.at[n], inc=1, device_id=dev(at(dz, 0)), device_id_type=MESH)

    for n in (10, 11, 12, 4, 5, 6, 7, 8, 9):
        loads[n].start()

    def send(src, dst, n, device, arrival=None):
        pltpu.make_async_remote_copy(
            src_ref=src,
            dst_ref=dst,
            send_sem=send_sem.at[n],
            recv_sem=recv_sem.at[n] if arrival is None else arrival,
            device_id=device,
            device_id_type=MESH,
        ).start()

    def arrived(view, n, arrival=None):
        pltpu.make_async_copy(view, view, recv_sem.at[n] if arrival is None else arrival).wait()

    def sent(view, n):
        pltpu.make_async_copy(view, view, send_sem.at[n]).wait()

    loads[0].wait()
    pl.semaphore_wait(barrier, len(near))
    tell(1, 0)
    wide = hidden[...].astype(F32)
    scale = lax.rsqrt(jnp.mean(wide * wide, -1, keepdims=True) + EPS)
    mine = hidden[:, pl.ds(pl.multiple_of(me * HD, HD), HD)].astype(F32)
    hid_cols[...] = mine
    normed_cols = (mine * scale).astype(BF16)
    for n in (1, 2, 3):
        loads[n].wait()
    width = group * HD
    for dx in (2, 1, 3, 0):
        g = lax.rem(x + dx, NX)
        part = jnp.dot(
            normed_cols,
            qw[:, pl.ds(pl.multiple_of(g * width, width), width)],
            preferred_element_type=F32,
        )
        for j in range(group):
            term[g, j] = part[:, j * HD : (j + 1) * HD]
        columns = pl.ds(pl.multiple_of(g * HD, HD), HD)
        term[g, group] = jnp.dot(normed_cols, kw[:, columns], preferred_element_type=F32)
        term[g, group + 1] = jnp.dot(normed_cols, vw[:, columns], preferred_element_type=F32)
        if dx:
            send(term.at[g], term_in.at[dx - 1], 0, dev(at(0, dx)))

    pl.semaphore_wait(here_sem.at[0], 2)
    tell(2, 1)
    pl.semaphore_wait(here_sem.at[1], 2)
    tell(4, 2)

    for n in (10, 11, 12):
        loads[n].wait()
    wide_pos = jnp.concatenate(
        [positions[k].astype(F32) for k in range(3)]
        + [jnp.zeros((HD - 3 * prompts, slots), F32)],
        0,
    )
    wide_pos = jnp.concatenate([wide_pos, jnp.zeros((HD, HD - slots), F32)], 1)
    pos_t[...] = wide_pos.T

    arrived(term_in, 0)
    for j in range(group + 2):
        item[:, j, :] = term[x, j] + term_in[0, j] + term_in[1, j] + term_in[2, j]

    pl.semaphore_wait(here_sem.at[2], 2)
    for dz in sorted(range(1, nz), key=lambda d: -min(d, nz - d)):
        p = lax.rem(z + dz, nz)
        send(item.at[p], item_in.at[dz - 1], 1, dev(at(dz, 0)))

    loads[4].wait()
    lane = lax.broadcasted_iota(jnp.int32, (slots, HD), 1)
    inv = inverse_row(lane)
    sign = jnp.where(lane < HD // 2, -1.0, 1.0)

    for p in range(prompts):
        ids = choose_ids(
            lane,
            pos_t[0:slots, p : p + 1],
            pos_t[0:slots, prompts + p : prompts + p + 1],
            pos_t[0:slots, 2 * prompts + p : 2 * prompts + p + 1],
        )
        angles = ids * inv
        cos_table = jnp.cos(angles)
        sin_table = jnp.sin(angles) * sign
        for g in range(kv):
            keys[p, g] = rotate(keys[p, g].astype(F32), cos_table, sin_table).astype(BF16)

    row = lax.broadcasted_iota(jnp.int32, (1, HD), 1)
    ids = choose_ids(
        row,
        query_pos[0, z].astype(F32),
        query_pos[1, z].astype(F32),
        query_pos[2, z].astype(F32),
    )
    angles = ids * inverse_row(row)
    cos_row = jnp.cos(angles)
    sin_row = jnp.sin(angles) * jnp.where(row < HD // 2, -1.0, 1.0)
    arrived(item_in, 1)
    total = item[z]
    for d in range(nz - 1):
        total = total + item_in[d]

    my_queries = rotate(total[0:group], cos_row, sin_row).astype(BF16)
    my_key = rotate(total[group : group + 1], cos_row, sin_row).astype(BF16).astype(F32)
    my_value = total[group + 1 : group + 2].astype(BF16).astype(F32)

    q_send[...] = my_queries
    q_all[me] = my_queries
    for dz in sorted(range(1, nz), key=lambda d: -min(d, nz - d)):
        send(q_send, q_all.at[me], 2, dev(at(dz, 0)), q_sem.at[dz])
    loads[5].wait()

    rows = kv * group
    r_i = lax.broadcasted_iota(jnp.int32, (rows, kv * slots), 0)
    c_i = lax.broadcasted_iota(jnp.int32, (rows, kv * slots), 1)
    diagonal = r_i // group == c_i // slots
    slot = c_i % slots + me * slots
    lane_minus_row = lax.broadcasted_iota(jnp.int32, (rows, HD), 1) - lax.broadcasted_iota(
        jnp.int32, (rows, HD), 0
    )
    mine_here = lax.broadcasted_iota(jnp.int32, (rows, 1), 0) // group == x

    def part_of(p, own):
        first = p * kv
        q4 = q_all[pl.ds(first, kv)].astype(F32).reshape(rows, HD)
        k4 = keys[p].reshape(kv * slots, HD)
        v4 = values[p].reshape(kv * slots, HD)
        scores = lax.dot_general(
            q4.astype(BF16), k4, (((1,), (1,)), ((), ())), preferred_element_type=F32
        ) * HD ** (-0.5)
        valid = diagonal & (slot < lengths[p])
        scores = jnp.where(valid, scores, -1e30)
        peak = jnp.max(scores, -1, keepdims=True)
        if own:
            own_score = jnp.sum(q4 * my_key[0], -1, keepdims=True) * HD ** (-0.5)
            peak = jnp.where(mine_here, jnp.maximum(peak, own_score), peak)
        weights = jnp.where(valid, jnp.exp(scores - peak), 0.0).astype(BF16)
        norm = jnp.sum(weights.astype(F32), -1, keepdims=True)
        blended = jnp.dot(weights, v4, preferred_element_type=F32)
        if own:
            own_weight = jnp.where(mine_here, jnp.exp(jnp.minimum(own_score - peak, 0.0)), 0.0)
            norm = norm + own_weight
            blended = blended + own_weight * my_value[0]
        some = norm > 0.0
        safe = jnp.where(some, norm, 1.0)
        lse = jnp.where(some, peak + jnp.log(safe), -1e30)
        blended = blended / safe
        o_send[p] = blended.reshape(kv, group, HD).astype(BF16)
        eye_lse = jnp.where(lane_minus_row == 0, lse, 0.0)
        lse_send[p] = jnp.sum(eye_lse, 0, keepdims=True)

    def away_at(near):
        return sorted({near, (nz - near) % nz})

    def relay(near):
        for dz in away_at(near):
            entry = lax.rem(z - dz + nz, nz) * kv + x
            if dz:
                arrived(q_all.at[pl.ds(0, 1)], 2, q_sem.at[dz])
            for dx in (2, 1, 3):
                send(q_all.at[entry], q_all.at[entry], 13, dev(at(0, dx)), q_x_sem.at[dz])

    def attend(near):
        away = away_at(near)
        for dz in away:
            arrived(q_all.at[pl.ds(0, NX - 1)], 13, q_x_sem.at[dz])
        for dz in away:
            part_of(lax.rem(z - dz + nz, nz), dz == 0)
        for dz in away:
            p = lax.rem(z - dz + nz, nz)
            if dz != nz // 2:
                owner = dev(at(nz - dz + nz // 2, 0))
                send(lse_send.at[p], lse_in.at[z], 3, owner)
                send(o_send.at[p], o_in.at[z], 4, owner)

    reach = nz // 2 + 1
    for near in range(reach + LAG):
        if near < reach:
            relay(near)
        if near >= LAG:
            attend(near - LAG)

    theirs = lax.rem(z + nz // 2, nz)
    o_in[z] = o_send[theirs]
    lse_in[z] = lse_send[theirs]
    arrived(lse_in.at[pl.ds(0, nz - 1)], 3)
    lse_rows = jnp.concatenate(
        [lse_in[...].reshape(nz, HD), jnp.full((HD - nz, HD), -1e30, F32)], 0
    )
    lse = lse_rows.T[0:rows]
    top = jnp.max(lse, -1, keepdims=True)
    factor = jnp.exp(lse - top)
    norm = jnp.sum(factor, -1, keepdims=True)
    factor = factor / norm
    joined_lse = top + jnp.log(norm)
    arrived(o_in.at[pl.ds(0, nz - 1)], 4)
    mixed = [None, None]
    for s in range(nz):
        piece = factor[:, s : s + 1] * o_in[s].astype(F32).reshape(rows, HD)
        k = s % 2
        mixed[k] = piece if mixed[k] is None else mixed[k] + piece
    join[x, 0:kv] = (mixed[0] + mixed[1]).reshape(kv, group, HD)
    head_lane = lax.broadcasted_iota(jnp.int32, (group, HD), 1)
    packed = jnp.zeros((group, HD), F32)
    for g in range(kv):
        packed = jnp.where(head_lane == g, joined_lse[g * group : (g + 1) * group], packed)
    join[x, kv] = packed

    for dx in (2, 1, 3):
        send(join.at[x], join.at[x], 5, dev(at(0, dx)))
    arrived(join.at[pl.ds(0, NX - 1)], 5)
    attended = []
    for g in range(kv):
        lse = [join[n, kv][:, g : g + 1] for n in range(NX)]
        top = jnp.maximum(jnp.maximum(lse[0], lse[1]), jnp.maximum(lse[2], lse[3]))
        factor = [jnp.exp(v - top) for v in lse]
        norm = (factor[0] + factor[1]) + (factor[2] + factor[3])
        total = sum(factor[n] * join[n, g] for n in range(NX)) / norm
        attended.append(total.astype(BF16))

    for g in range(kv):
        att_all[theirs, g] = attended[g]
    for dz in sorted(range(1, nz), key=lambda d: -min(d, nz - d)):
        send(att_all.at[theirs], att_all.at[theirs], 12, dev(at(dz, 0)))
    loads[6].wait()
    arrived(att_all.at[pl.ds(0, nz - 1)], 12)
    att_rows[...] = att_all[...].astype(F32).reshape(pool * group, HD)
    for j in range(rows):
        att_lhs[:, j * HD : (j + 1) * HD] = att_rows[
            pl.ds(j, prompts, stride=rows), :
        ].astype(BF16)
    projected = jnp.dot(att_lhs[...], ow[...], preferred_element_type=F32)

    proj[0] = projected[0:half]
    proj[1] = projected[half:prompts]
    send(proj.at[1 - core], proj_in, 6, other)
    arrived(proj_in, 6)
    mid = (
        hid_cols[pl.ds(pl.multiple_of(core * half, half), half), :] + proj[core] + proj_in[...]
    ).astype(BF16)

    mid_send[...] = mid
    for dz, dx in steps:
        send(mid_send, mid_all.at[core, me], 7, dev(at(dz, dx)))
    mid_all[core, me] = mid
    arrived(mid_all.at[0, pl.ds(0, pool - 1)], 7)
    send(mid_all.at[core], mid_all.at[core], 8, other)

    def scale_of(half_of):
        state = mid_all[half_of].astype(F32)
        squares = jnp.sum(jnp.sum(state * state, 0), -1, keepdims=True)
        return lax.rsqrt(squares * (1.0 / (pool * HD)) + EPS)

    my_scale = scale_of(core)
    arrived(mid_all.at[0], 8)
    their_scale = scale_of(1 - core)
    inverse = [jnp.where(core == c, my_scale, their_scale) for c in range(2)]
    for k in range(pool):
        chunk = jnp.concatenate([mid_all[c, k].astype(F32) * inverse[c] for c in range(2)], 0)
        normed_lhs[:, k * HD : (k + 1) * HD] = chunk.astype(BF16)
    loads[7].wait()
    loads[8].wait()
    across = (((1,), (1,)), ((), ()))
    gate = lax.dot_general(normed_lhs[...], gw[...], across, preferred_element_type=F32)
    up = lax.dot_general(normed_lhs[...], uw[...], across, preferred_element_type=F32)
    active = (gate / (1.0 + jnp.exp(-gate)) * up).astype(BF16)

    loads[9].wait()
    order = sorted(range(nz), key=lambda d: -min(d, nz - d))

    def down_columns(n):
        for dz in order[n * NX : (n + 1) * NX]:
            first = lax.rem(z + dz, nz) * NX
            part = jnp.dot(
                active,
                dw[:, pl.ds(pl.multiple_of(first * HD, NX * HD), NX * HD)],
                preferred_element_type=F32,
            )
            at_n = (n * NX + order[n * NX : (n + 1) * NX].index(dz)) * NX
            for k in range(NX):
                down[0, at_n + k] = part[0:half, k * HD : (k + 1) * HD]
                down[1, at_n + k] = part[half:prompts, k * HD : (k + 1) * HD]
        block = pl.ds(n * NX * NX, NX * NX)
        send(down.at[1 - core, block], down_in.at[block], 9, other, down_sem.at[n])

    def down_out(n):
        block = pl.ds(n * NX * NX, NX * NX)
        arrived(down_in.at[block], 9, down_sem.at[n])
        down_send[block] = (down[core, block] + down_in[block]).astype(BF16)
        for i, dz in enumerate(order[n * NX : (n + 1) * NX]):
            for dx in (2, 1, 3, 0):
                if dz == 0 and dx == 0:
                    continue
                entry = (n * NX + i) * NX + lax.rem(x + dx, NX)
                send(down_send.at[entry], part_in.at[dz * NX + dx - 1], 10, dev(at(dz, dx)))

    down_columns(0)
    down_columns(1)
    for n in range(2, nz // NX):
        down_out(n - 2)
        down_columns(n)
    down_out(nz // NX - 2)
    down_out(nz // NX - 1)
    part_in[pool - 1] = down_send[(nz - 1) * NX + x]
    arrived(part_in.at[pl.ds(0, pool - 1)], 10)
    done = mid.astype(F32) + jnp.sum(part_in[...].astype(F32), 0)
    fin[core] = done.astype(BF16)
    send(fin.at[core], fin.at[core], 11, other)
    arrived(fin.at[0], 11)
    out_ref[...] = jnp.concatenate([fin[0].astype(F32), fin[1].astype(F32)], 0).astype(BF16)

    sent(term_in, 0)
    sent(item_in, 1)
    sent(q_all.at[pl.ds(0, nz - 1)], 2)
    sent(q_all.at[pl.ds(0, nz * (NX - 1))], 13)
    sent(lse_in.at[pl.ds(0, nz - 1)], 3)
    sent(o_in.at[pl.ds(0, nz - 1)], 4)
    sent(join.at[pl.ds(0, NX - 1)], 5)
    sent(att_all.at[pl.ds(0, nz - 1)], 12)
    sent(proj_in, 6)
    sent(mid_all.at[0, pl.ds(0, pool - 1)], 7)
    sent(mid_all.at[0], 8)
    sent(down_in, 9)
    sent(part_in.at[pl.ds(0, pool - 1)], 10)
    sent(fin.at[0], 11)


def solution(mesh):
    pool = mesh.shape["pool"]

    def per_device(
        hidden_in,
        key_cache,
        value_cache,
        positions,
        query_pos,
        lengths,
        query_weight,
        key_weight,
        value_weight,
        out_weight,
        gate_weight,
        up_weight,
        down_weight,
    ):
        gate_weight, up_weight = gate_weight.T, up_weight.T
        prompts, kv, slots, _ = key_cache.shape
        group = query_weight.shape[1] // (kv * HD)
        nz = pool // NX
        parts = group + 2
        half = prompts // 2
        hbm = pl.BlockSpec(memory_space=pltpu.HBM)
        vmem = pl.BlockSpec(memory_space=pltpu.VMEM)

        def like(a):
            return pltpu.VMEM(a.shape, a.dtype)

        scratch = [
            pltpu.SMEM(query_pos.shape, jnp.int32),
            pltpu.SMEM(lengths.shape, jnp.int32),
            like(positions),
            like(hidden_in),
            like(key_cache),
            like(value_cache),
            like(query_weight),
            like(key_weight),
            like(value_weight),
            like(out_weight),
            like(gate_weight),
            like(up_weight),
            like(down_weight),
            pltpu.VMEM((kv, parts, prompts, HD), F32),
            pltpu.VMEM((NX - 1, parts, prompts, HD), F32),
            pltpu.VMEM((prompts, parts, HD), F32),
            pltpu.VMEM((nz - 1, parts, HD), F32),
            pltpu.VMEM((group, HD), BF16),
            pltpu.VMEM((pool, group, HD), BF16),
            pltpu.VMEM((HD, HD), F32),
            pltpu.VMEM((prompts, kv, group, HD), BF16),
            pltpu.VMEM((nz, kv, group, HD), BF16),
            pltpu.VMEM((prompts, 1, HD), F32),
            pltpu.VMEM((nz, 1, HD), F32),
            pltpu.VMEM((NX, kv + 1, group, HD), F32),
            pltpu.VMEM((prompts, kv, group, HD), BF16),
            pltpu.VMEM((pool * group, HD), F32),
            pltpu.VMEM((prompts, kv * group * HD), BF16),
            pltpu.VMEM((prompts, HD), F32),
            pltpu.VMEM((2, half, HD), F32),
            pltpu.VMEM((half, HD), F32),
            pltpu.VMEM((half, HD), BF16),
            pltpu.VMEM((2, pool, half, HD), BF16),
            pltpu.VMEM((prompts, pool * HD), BF16),
            pltpu.VMEM((2, pool, half, HD), F32),
            pltpu.VMEM((pool, half, HD), F32),
            pltpu.VMEM((pool, half, HD), BF16),
            pltpu.VMEM((pool, half, HD), BF16),
            pltpu.VMEM((2, half, HD), BF16),
            pltpu.SemaphoreType.DMA((13,)),
            pltpu.SemaphoreType.DMA((14,)),
            pltpu.SemaphoreType.DMA((14,)),
            pltpu.SemaphoreType.REGULAR((3,)),
            pltpu.SemaphoreType.DMA((nz,)),
            pltpu.SemaphoreType.DMA((nz // NX,)),
            pltpu.SemaphoreType.DMA((nz,)),
        ]
        return pl.pallas_call(
            functools.partial(body, (prompts, pool, kv, group, slots)),
            out_shape=jax.ShapeDtypeStruct((prompts, HD), BF16),
            in_specs=[hbm] * 13,
            out_specs=vmem,
            scratch_shapes=scratch,
            compiler_params=pltpu.CompilerParams(
                collective_id=0, has_side_effects=True, vmem_limit_bytes=60 * 1024 * 1024
            ),
        )(
            query_pos,
            lengths,
            hidden_in,
            key_cache,
            value_cache,
            positions,
            query_weight,
            key_weight,
            value_weight,
            out_weight,
            gate_weight,
            up_weight,
            down_weight,
        )

    in_specs = (
        P("groups", None),
        P("groups", "heads", "pool", None),
        P("groups", "heads", "pool", None),
        P(None, "groups", "pool"),
        P(None, "groups"),
        P("groups"),
        P("pool", "heads"),
        P("pool", "heads"),
        P("pool", "heads"),
        P("heads", "pool"),
        P(None, ("pool", "heads")),
        P(None, ("pool", "heads")),
        P(("pool", "heads"), None),
    )
    return jax.shard_map(
        per_device, mesh=mesh, in_specs=in_specs, out_specs=P("groups", "pool"), check_vma=False
    )
```

```python
import functools
import math

import jax
import jax.numpy as jnp
from jax import lax
from jax.experimental import pallas as pl
from jax.experimental.pallas import tpu as pltpu
from jax.sharding import PartitionSpec as P

HD = 128
EPS = 1e-06
THETA = 1000000.0
LAG = 6
NX = 4
MESH = pl.DeviceIdType.MESH
F32 = jnp.float32
BF16 = jnp.bfloat16


def far_first(pool):
    nz = pool // NX
    steps = [(a, b) for a in range(nz) for b in range(NX) if (a, b) != (0, 0)]
    return sorted(steps, key=lambda s: -(min(s[0], nz - s[0]) + min(s[1], NX - s[1])))


def rotate(values, cos_table, sin_table):
    return values * cos_table + pltpu.roll(values, HD // 2, values.ndim - 1) * sin_table


def choose_ids(lane, t, h, w):
    column = lane % (HD // 2)
    first_end = HD // 8
    second_end = first_end + 3 * HD // 16
    return jnp.where(column < first_end, t, jnp.where(column < second_end, h, w))


def inverse_row(lane):
    column = (lane % (HD // 2)).astype(F32)
    return jnp.exp(column * (-2.0 * math.log(THETA) / HD))


def body(
    cfg,
    query_pos_hbm,
    lengths_hbm,
    hidden_hbm,
    key_hbm,
    value_hbm,
    positions_hbm,
    qw_hbm,
    kw_hbm,
    vw_hbm,
    ow_hbm,
    gw_hbm,
    uw_hbm,
    dw_hbm,
    out_ref,
    query_pos,
    lengths,
    positions,
    hidden,
    keys,
    values,
    qw,
    kw,
    vw,
    ow,
    gw,
    uw,
    dw,
    term,
    term_in,
    item,
    item_in,
    q_send,
    q_all,
    pos_t,
    o_send,
    o_in,
    lse_send,
    lse_in,
    join,
    att_all,
    att_rows,
    att_lhs,
    hid_cols,
    proj,
    proj_in,
    mid_send,
    mid_all,
    normed_lhs,
    down,
    down_in,
    down_send,
    part_in,
    fin,
    load_sem,
    send_sem,
    recv_sem,
    here_sem,
    q_sem,
    down_sem,
    q_x_sem,
):
    prompts, pool, kv, group, slots = cfg
    nz = pool // NX
    group_i = lax.axis_index("groups")
    me = lax.axis_index("pool")
    core = lax.axis_index("heads")
    z = me // NX
    x = me % NX
    half = prompts // 2
    steps = far_first(pool)

    def at(dz, dx):
        return lax.rem(z + dz, nz) * NX + lax.rem(x + dx, NX)

    def dev(p):
        return (group_i, p, core)

    other = (group_i, me, 1 - core)

    loads = []
    for n, (src, dst) in enumerate(
        [
            (hidden_hbm, hidden),
            (qw_hbm, qw),
            (kw_hbm, kw),
            (vw_hbm, vw),
            (key_hbm, keys),
            (value_hbm, values),
            (ow_hbm, ow),
            (gw_hbm, gw),
            (uw_hbm, uw),
            (dw_hbm, dw),
            (positions_hbm, positions),
            (query_pos_hbm, query_pos),
            (lengths_hbm, lengths),
        ]
    ):
        copy = pltpu.make_async_copy(src, dst, load_sem.at[n])
        loads.append(copy)
    for n in (0, 1, 2, 3):
        loads[n].start()


    barrier = pltpu.get_barrier_semaphore()
    near = [dev(at(0, dx)) for dx in (2, 1, 3)] + [dev(at(1, 0)), dev(at(nz - 1, 0)), other]
    for device in near:
        pl.semaphore_signal(barrier, inc=1, device_id=device, device_id_type=MESH)

    def tell(distance, n):
        for dz in (distance, nz - distance):
            pl.semaphore_signal(here_sem.at[n], inc=1, device_id=dev(at(dz, 0)), device_id_type=MESH)

    for n in (10, 11, 12, 4, 5, 6, 7, 8, 9):
        loads[n].start()

    def send(src, dst, n, device, arrival=None):
        pltpu.make_async_remote_copy(
            src_ref=src,
            dst_ref=dst,
            send_sem=send_sem.at[n],
            recv_sem=recv_sem.at[n] if arrival is None else arrival,
            device_id=device,
            device_id_type=MESH,
        ).start()

    def arrived(view, n, arrival=None):
        pltpu.make_async_copy(view, view, recv_sem.at[n] if arrival is None else arrival).wait()

    def sent(view, n):
        pltpu.make_async_copy(view, view, send_sem.at[n]).wait()

    loads[0].wait()
    pl.semaphore_wait(barrier, len(near))
    tell(1, 0)
    wide = hidden[...].astype(F32)
    scale = lax.rsqrt(jnp.mean(wide * wide, -1, keepdims=True) + EPS)
    mine = hidden[:, pl.ds(pl.multiple_of(me * HD, HD), HD)].astype(F32)
    hid_cols[...] = mine
    normed_cols = (mine * scale).astype(BF16)
    for n in (1, 2, 3):
        loads[n].wait()
    width = group * HD
    for dx in (2, 1, 3, 0):
        g = lax.rem(x + dx, NX)
        part = jnp.dot(
            normed_cols,
            qw[:, pl.ds(pl.multiple_of(g * width, width), width)],
            preferred_element_type=F32,
        )
        for j in range(group):
            term[g, j] = part[:, j * HD : (j + 1) * HD]
        columns = pl.ds(pl.multiple_of(g * HD, HD), HD)
        term[g, group] = jnp.dot(normed_cols, kw[:, columns], preferred_element_type=F32)
        term[g, group + 1] = jnp.dot(normed_cols, vw[:, columns], preferred_element_type=F32)
        if dx:
            send(term.at[g], term_in.at[dx - 1], 0, dev(at(0, dx)))

    pl.semaphore_wait(here_sem.at[0], 2)
    tell(2, 1)
    pl.semaphore_wait(here_sem.at[1], 2)
    tell(4, 2)

    for n in (10, 11, 12):
        loads[n].wait()
    wide_pos = jnp.concatenate(
        [positions[k].astype(F32) for k in range(3)]
        + [jnp.zeros((HD - 3 * prompts, slots), F32)],
        0,
    )
    wide_pos = jnp.concatenate([wide_pos, jnp.zeros((HD, HD - slots), F32)], 1)
    pos_t[...] = wide_pos.T

    arrived(term_in, 0)
    for j in range(group + 2):
        item[:, j, :] = term[x, j] + term_in[0, j] + term_in[1, j] + term_in[2, j]

    pl.semaphore_wait(here_sem.at[2], 2)
    for dz in sorted(range(1, nz), key=lambda d: -min(d, nz - d)):
        p = lax.rem(z + dz, nz)
        send(item.at[p], item_in.at[dz - 1], 1, dev(at(dz, 0)))

    loads[4].wait()
    lane = lax.broadcasted_iota(jnp.int32, (slots, HD), 1)
    inv = inverse_row(lane)
    sign = jnp.where(lane < HD // 2, -1.0, 1.0)

    for p in range(prompts):
        ids = choose_ids(
            lane,
            pos_t[0:slots, p : p + 1],
            pos_t[0:slots, prompts + p : prompts + p + 1],
            pos_t[0:slots, 2 * prompts + p : 2 * prompts + p + 1],
        )
        angles = ids * inv
        cos_table = jnp.cos(angles)
        sin_table = jnp.sin(angles) * sign
        for g in range(kv):
            keys[p, g] = rotate(keys[p, g].astype(F32), cos_table, sin_table).astype(BF16)

    arrived(item_in, 1)
    total = item[z]
    for d in range(nz - 1):
        total = total + item_in[d]

    row = lax.broadcasted_iota(jnp.int32, (1, HD), 1)
    ids = choose_ids(
        row,
        query_pos[0, z].astype(F32),
        query_pos[1, z].astype(F32),
        query_pos[2, z].astype(F32),
    )
    angles = ids * inverse_row(row)
    cos_row = jnp.cos(angles)
    sin_row = jnp.sin(angles) * jnp.where(row < HD // 2, -1.0, 1.0)
    my_queries = rotate(total[0:group], cos_row, sin_row).astype(BF16)
    my_key = rotate(total[group : group + 1], cos_row, sin_row).astype(BF16).astype(F32)
    my_value = total[group + 1 : group + 2].astype(BF16).astype(F32)

    q_send[...] = my_queries
    q_all[me] = my_queries
    for dz in sorted(range(1, nz), key=lambda d: min(d, nz - d)):
        send(q_send, q_all.at[me], 2, dev(at(dz, 0)), q_sem.at[dz])
    loads[5].wait()

    rows = kv * group
    r_i = lax.broadcasted_iota(jnp.int32, (rows, kv * slots), 0)
    c_i = lax.broadcasted_iota(jnp.int32, (rows, kv * slots), 1)
    diagonal = r_i // group == c_i // slots
    slot = c_i % slots + me * slots
    lane_minus_row = lax.broadcasted_iota(jnp.int32, (rows, HD), 1) - lax.broadcasted_iota(
        jnp.int32, (rows, HD), 0
    )
    mine_here = lax.broadcasted_iota(jnp.int32, (rows, 1), 0) // group == x

    def part_of(p, own):
        first = p * kv
        q4 = q_all[pl.ds(first, kv)].astype(F32).reshape(rows, HD)
        k4 = keys[p].reshape(kv * slots, HD)
        v4 = values[p].reshape(kv * slots, HD)
        scores = lax.dot_general(
            q4.astype(BF16), k4, (((1,), (1,)), ((), ())), preferred_element_type=F32
        ) * HD ** (-0.5)
        valid = diagonal & (slot < lengths[p])
        scores = jnp.where(valid, scores, -1e30)
        peak = jnp.max(scores, -1, keepdims=True)
        if own:
            own_score = jnp.sum(q4 * my_key[0], -1, keepdims=True) * HD ** (-0.5)
            peak = jnp.where(mine_here, jnp.maximum(peak, own_score), peak)
        weights = jnp.where(valid, jnp.exp(scores - peak), 0.0).astype(BF16)
        norm = jnp.sum(weights.astype(F32), -1, keepdims=True)
        blended = jnp.dot(weights, v4, preferred_element_type=F32)
        if own:
            own_weight = jnp.where(mine_here, jnp.exp(jnp.minimum(own_score - peak, 0.0)), 0.0)
            norm = norm + own_weight
            blended = blended + own_weight * my_value[0]
        some = norm > 0.0
        safe = jnp.where(some, norm, 1.0)
        lse = jnp.where(some, peak + jnp.log(safe), -1e30)
        blended = blended / safe
        o_send[p] = blended.reshape(kv, group, HD).astype(BF16)
        eye_lse = jnp.where(lane_minus_row == 0, lse, 0.0)
        lse_send[p] = jnp.sum(eye_lse, 0, keepdims=True)

    def away_at(near):
        return sorted({near, (nz - near) % nz})

    def relay(near):
        for dz in away_at(near):
            entry = lax.rem(z - dz + nz, nz) * kv + x
            if dz:
                arrived(q_all.at[pl.ds(0, 1)], 2, q_sem.at[dz])
            for dx in (2, 1, 3):
                send(q_all.at[entry], q_all.at[entry], 13, dev(at(0, dx)), q_x_sem.at[dz])

    def attend(near):
        away = away_at(near)
        for dz in away:
            arrived(q_all.at[pl.ds(0, NX - 1)], 13, q_x_sem.at[dz])
        for dz in away:
            part_of(lax.rem(z - dz + nz, nz), dz == 0)
        for dz in away:
            p = lax.rem(z - dz + nz, nz)
            if dz != nz // 2:
                owner = dev(at(nz - dz + nz // 2, 0))
                send(lse_send.at[p], lse_in.at[z], 3, owner)
                send(o_send.at[p], o_in.at[z], 4, owner)

    reach = nz // 2 + 1
    for near in range(reach + LAG):
        if near < reach:
            relay(near)
        if near >= LAG:
            attend(near - LAG)

    theirs = lax.rem(z + nz // 2, nz)
    o_in[z] = o_send[theirs]
    lse_in[z] = lse_send[theirs]
    arrived(lse_in.at[pl.ds(0, nz - 1)], 3)
    lse_rows = jnp.concatenate(
        [lse_in[...].reshape(nz, HD), jnp.full((HD - nz, HD), -1e30, F32)], 0
    )
    lse = lse_rows.T[0:rows]
    top = jnp.max(lse, -1, keepdims=True)
    factor = jnp.exp(lse - top)
    norm = jnp.sum(factor, -1, keepdims=True)
    factor = factor / norm
    joined_lse = top + jnp.log(norm)
    arrived(o_in.at[pl.ds(0, nz - 1)], 4)
    mixed = [None, None]
    for s in range(nz):
        piece = factor[:, s : s + 1] * o_in[s].astype(F32).reshape(rows, HD)
        k = s % 2
        mixed[k] = piece if mixed[k] is None else mixed[k] + piece
    join[x, 0:kv] = (mixed[0] + mixed[1]).reshape(kv, group, HD)
    head_lane = lax.broadcasted_iota(jnp.int32, (group, HD), 1)
    packed = jnp.zeros((group, HD), F32)
    for g in range(kv):
        packed = jnp.where(head_lane == g, joined_lse[g * group : (g + 1) * group], packed)
    join[x, kv] = packed

    for dx in (2, 1, 3):
        send(join.at[x], join.at[x], 5, dev(at(0, dx)))
    arrived(join.at[pl.ds(0, NX - 1)], 5)
    attended = []
    for g in range(kv):
        lse = [join[n, kv][:, g : g + 1] for n in range(NX)]
        top = jnp.maximum(jnp.maximum(lse[0], lse[1]), jnp.maximum(lse[2], lse[3]))
        factor = [jnp.exp(v - top) for v in lse]
        norm = (factor[0] + factor[1]) + (factor[2] + factor[3])
        total = sum(factor[n] * join[n, g] for n in range(NX)) / norm
        attended.append(total.astype(BF16))

    for g in range(kv):
        att_all[theirs, g] = attended[g]
    for dz in sorted(range(1, nz), key=lambda d: -min(d, nz - d)):
        send(att_all.at[theirs], att_all.at[theirs], 12, dev(at(dz, 0)))
    loads[6].wait()
    arrived(att_all.at[pl.ds(0, nz - 1)], 12)
    att_rows[...] = att_all[...].astype(F32).reshape(pool * group, HD)
    for j in range(rows):
        att_lhs[:, j * HD : (j + 1) * HD] = att_rows[
            pl.ds(j, prompts, stride=rows), :
        ].astype(BF16)
    projected = jnp.dot(att_lhs[...], ow[...], preferred_element_type=F32)

    proj[0] = projected[0:half]
    proj[1] = projected[half:prompts]
    send(proj.at[1 - core], proj_in, 6, other)
    arrived(proj_in, 6)
    mid = (
        hid_cols[pl.ds(pl.multiple_of(core * half, half), half), :] + proj[core] + proj_in[...]
    ).astype(BF16)

    mid_send[...] = mid
    for dz, dx in steps:
        send(mid_send, mid_all.at[core, me], 7, dev(at(dz, dx)))
    mid_all[core, me] = mid
    arrived(mid_all.at[0, pl.ds(0, pool - 1)], 7)
    send(mid_all.at[core], mid_all.at[core], 8, other)
    arrived(mid_all.at[0], 8)

    inverse = []
    for c in range(2):
        state = mid_all[c].astype(F32)
        squares = jnp.sum(jnp.sum(state * state, 0), -1, keepdims=True)
        inverse.append(lax.rsqrt(squares * (1.0 / (pool * HD)) + EPS))
    for k in range(pool):
        chunk = jnp.concatenate([mid_all[c, k].astype(F32) * inverse[c] for c in range(2)], 0)
        normed_lhs[:, k * HD : (k + 1) * HD] = chunk.astype(BF16)
    loads[7].wait()
    loads[8].wait()
    across = (((1,), (1,)), ((), ()))
    gate = lax.dot_general(normed_lhs[...], gw[...], across, preferred_element_type=F32)
    up = lax.dot_general(normed_lhs[...], uw[...], across, preferred_element_type=F32)
    active = (gate / (1.0 + jnp.exp(-gate)) * up).astype(BF16)

    loads[9].wait()
    order = sorted(range(nz), key=lambda d: -min(d, nz - d))

    def down_columns(n):
        for dz in order[n * NX : (n + 1) * NX]:
            first = lax.rem(z + dz, nz) * NX
            part = jnp.dot(
                active,
                dw[:, pl.ds(pl.multiple_of(first * HD, NX * HD), NX * HD)],
                preferred_element_type=F32,
            )
            at_n = (n * NX + order[n * NX : (n + 1) * NX].index(dz)) * NX
            for k in range(NX):
                down[0, at_n + k] = part[0:half, k * HD : (k + 1) * HD]
                down[1, at_n + k] = part[half:prompts, k * HD : (k + 1) * HD]
        block = pl.ds(n * NX * NX, NX * NX)
        send(down.at[1 - core, block], down_in.at[block], 9, other, down_sem.at[n])

    def down_out(n):
        block = pl.ds(n * NX * NX, NX * NX)
        arrived(down_in.at[block], 9, down_sem.at[n])
        down_send[block] = (down[core, block] + down_in[block]).astype(BF16)
        for i, dz in enumerate(order[n * NX : (n + 1) * NX]):
            for dx in (2, 1, 3, 0):
                if dz == 0 and dx == 0:
                    continue
                entry = (n * NX + i) * NX + lax.rem(x + dx, NX)
                send(down_send.at[entry], part_in.at[dz * NX + dx - 1], 10, dev(at(dz, dx)))

    down_columns(0)
    down_columns(1)
    for n in range(2, nz // NX):
        down_out(n - 2)
        down_columns(n)
    down_out(nz // NX - 2)
    down_out(nz // NX - 1)
    part_in[pool - 1] = down_send[(nz - 1) * NX + x]
    arrived(part_in.at[pl.ds(0, pool - 1)], 10)
    done = mid.astype(F32) + jnp.sum(part_in[...].astype(F32), 0)
    fin[core] = done.astype(BF16)
    send(fin.at[core], fin.at[core], 11, other)
    arrived(fin.at[0], 11)
    out_ref[...] = jnp.concatenate([fin[0].astype(F32), fin[1].astype(F32)], 0).astype(BF16)

    sent(term_in, 0)
    sent(item_in, 1)
    sent(q_all.at[pl.ds(0, nz - 1)], 2)
    sent(q_all.at[pl.ds(0, nz * (NX - 1))], 13)
    sent(lse_in.at[pl.ds(0, nz - 1)], 3)
    sent(o_in.at[pl.ds(0, nz - 1)], 4)
    sent(join.at[pl.ds(0, NX - 1)], 5)
    sent(att_all.at[pl.ds(0, nz - 1)], 12)
    sent(proj_in, 6)
    sent(mid_all.at[0, pl.ds(0, pool - 1)], 7)
    sent(mid_all.at[0], 8)
    sent(down_in, 9)
    sent(part_in.at[pl.ds(0, pool - 1)], 10)
    sent(fin.at[0], 11)


def solution(mesh):
    pool = mesh.shape["pool"]

    def per_device(
        hidden_in,
        key_cache,
        value_cache,
        positions,
        query_pos,
        lengths,
        query_weight,
        key_weight,
        value_weight,
        out_weight,
        gate_weight,
        up_weight,
        down_weight,
    ):
        gate_weight, up_weight = gate_weight.T, up_weight.T
        prompts, kv, slots, _ = key_cache.shape
        group = query_weight.shape[1] // (kv * HD)
        nz = pool // NX
        parts = group + 2
        half = prompts // 2
        hbm = pl.BlockSpec(memory_space=pltpu.HBM)
        vmem = pl.BlockSpec(memory_space=pltpu.VMEM)

        def like(a):
            return pltpu.VMEM(a.shape, a.dtype)

        scratch = [
            pltpu.SMEM(query_pos.shape, jnp.int32),
            pltpu.SMEM(lengths.shape, jnp.int32),
            like(positions),
            like(hidden_in),
            like(key_cache),
            like(value_cache),
            like(query_weight),
            like(key_weight),
            like(value_weight),
            like(out_weight),
            like(gate_weight),
            like(up_weight),
            like(down_weight),
            pltpu.VMEM((kv, parts, prompts, HD), F32),
            pltpu.VMEM((NX - 1, parts, prompts, HD), F32),
            pltpu.VMEM((prompts, parts, HD), F32),
            pltpu.VMEM((nz - 1, parts, HD), F32),
            pltpu.VMEM((group, HD), BF16),
            pltpu.VMEM((pool, group, HD), BF16),
            pltpu.VMEM((HD, HD), F32),
            pltpu.VMEM((prompts, kv, group, HD), BF16),
            pltpu.VMEM((nz, kv, group, HD), BF16),
            pltpu.VMEM((prompts, 1, HD), F32),
            pltpu.VMEM((nz, 1, HD), F32),
            pltpu.VMEM((NX, kv + 1, group, HD), F32),
            pltpu.VMEM((prompts, kv, group, HD), BF16),
            pltpu.VMEM((pool * group, HD), F32),
            pltpu.VMEM((prompts, kv * group * HD), BF16),
            pltpu.VMEM((prompts, HD), F32),
            pltpu.VMEM((2, half, HD), F32),
            pltpu.VMEM((half, HD), F32),
            pltpu.VMEM((half, HD), BF16),
            pltpu.VMEM((2, pool, half, HD), BF16),
            pltpu.VMEM((prompts, pool * HD), BF16),
            pltpu.VMEM((2, pool, half, HD), F32),
            pltpu.VMEM((pool, half, HD), F32),
            pltpu.VMEM((pool, half, HD), BF16),
            pltpu.VMEM((pool, half, HD), BF16),
            pltpu.VMEM((2, half, HD), BF16),
            pltpu.SemaphoreType.DMA((13,)),
            pltpu.SemaphoreType.DMA((14,)),
            pltpu.SemaphoreType.DMA((14,)),
            pltpu.SemaphoreType.REGULAR((3,)),
            pltpu.SemaphoreType.DMA((nz,)),
            pltpu.SemaphoreType.DMA((nz // NX,)),
            pltpu.SemaphoreType.DMA((nz,)),
        ]
        return pl.pallas_call(
            functools.partial(body, (prompts, pool, kv, group, slots)),
            out_shape=jax.ShapeDtypeStruct((prompts, HD), BF16),
            in_specs=[hbm] * 13,
            out_specs=vmem,
            scratch_shapes=scratch,
            compiler_params=pltpu.CompilerParams(
                collective_id=0, has_side_effects=True, vmem_limit_bytes=60 * 1024 * 1024
            ),
        )(
            query_pos,
            lengths,
            hidden_in,
            key_cache,
            value_cache,
            positions,
            query_weight,
            key_weight,
            value_weight,
            out_weight,
            gate_weight,
            up_weight,
            down_weight,
        )

    in_specs = (
        P("groups", None),
        P("groups", "heads", "pool", None),
        P("groups", "heads", "pool", None),
        P(None, "groups", "pool"),
        P(None, "groups"),
        P("groups"),
        P("pool", "heads"),
        P("pool", "heads"),
        P("pool", "heads"),
        P("heads", "pool"),
        P(None, ("pool", "heads")),
        P(None, ("pool", "heads")),
        P(("pool", "heads"), None),
    )
    return jax.shard_map(
        per_device, mesh=mesh, in_specs=in_specs, out_specs=P("groups", "pool"), check_vma=False
    )
```
